16 devices in a mesh: fsdp: 16 (over z, y, x, core).
Axes of the slice: x: 2, y: 2, z: 2, core: 2. Of those that a mesh axis runs over, the one named last changes fastest.
Arguments:
- hidden: bfloat16 [5, 16384, 576], P(None, 'fsdp')
- w_gate: bfloat16 [5, 576, 1536], P(None, 'fsdp')
- w_up: bfloat16 [5, 576, 1536], P(None, 'fsdp')
- w_down: bfloat16 [5, 1536, 576], P(None, 'fsdp')
- w_out: bfloat16 [576, 49152], P('fsdp')
- targets: int32 [16384], P('fsdp')
- loss_mask: int32 [16384], P('fsdp')
Outputs:
- output 1: float32 [5, 576, 1536], P(None, 'fsdp')
- output 2: float32 [5, 576, 1536], P(None, 'fsdp')
- output 3: float32 [5, 1536, 576], P(None, 'fsdp')
- output 4: float32 [576, 49152], P('fsdp')
- output 5: bfloat16 [16384, 576], P('fsdp')
- output 6: float32 [], replicated
All inputs are finite; a program needn't handle non-finite values.
Results may differ from the reference program's by a relative error of at most 0.0137025.
Values are sent between devices in bfloat16 or wider.
A program may use at most 1 GiB of HBM per device.

```python
import jax
import jax.numpy as jnp
from jax import lax

LAYERS = 5
TOK_DEV = 1024
GROUP_SIZE = 16
HIDDEN = 576
FFN_DIM = 1536
VOCAB_SIZE = 49152
TOKENS = 16384

NORM_EPS = 1e-5


def draw_labels(label_key):
    key_tgt, key_rate, key_keep = jax.random.split(label_key, 3)
    targets = jax.random.randint(key_tgt, (TOKENS,), 0, VOCAB_SIZE, dtype=jnp.int32)
    targets = targets.at[0].set(VOCAB_SIZE - 1)
    keep_rate = jax.random.randint(key_rate, (GROUP_SIZE, 1), 2, 17, dtype=jnp.int32)
    ticket = jax.random.randint(key_keep, (GROUP_SIZE, TOK_DEV), 0, 16, dtype=jnp.int32)
    loss_mask = (ticket < keep_rate).astype(jnp.int32).reshape(TOKENS)
    loss_mask = loss_mask.at[0].set(1)
    return targets, loss_mask


def setup_inputs(seed: int = 0) -> dict:
    sub_keys = jax.random.split(jax.random.key(seed), 6)
    hidden = jax.random.normal(sub_keys[0], (LAYERS, TOKENS, HIDDEN), jnp.float32).astype(jnp.bfloat16)
    w_gate = (jax.random.normal(sub_keys[1], (LAYERS, HIDDEN, FFN_DIM), jnp.float32) * HIDDEN ** -0.5).astype(jnp.bfloat16)
    w_up = (jax.random.normal(sub_keys[2], (LAYERS, HIDDEN, FFN_DIM), jnp.float32) * HIDDEN ** -0.5).astype(jnp.bfloat16)
    w_down = (jax.random.normal(sub_keys[3], (LAYERS, FFN_DIM, HIDDEN), jnp.float32) * FFN_DIM ** -0.5).astype(jnp.bfloat16)
    w_out = (jax.random.normal(sub_keys[4], (HIDDEN, VOCAB_SIZE), jnp.float32) * HIDDEN ** -0.5).astype(jnp.bfloat16)
    targets, loss_mask = draw_labels(sub_keys[5])
    return {'hidden': hidden, 'w_gate': w_gate, 'w_up': w_up, 'w_down': w_down, 'w_out': w_out, 'targets': targets, 'loss_mask': loss_mask}


def norm_apply(x_in):
    x_f32 = x_in.astype(jnp.float32)
    inv_rms = lax.rsqrt(jnp.mean(x_f32 * x_f32, axis=-1, keepdims=True) + NORM_EPS)
    return (x_f32 * inv_rms).astype(jnp.bfloat16)


def norm_grad(x_in, grad_y):
    x_f32 = x_in.astype(jnp.float32)
    inv_rms = lax.rsqrt(jnp.mean(x_f32 * x_f32, axis=-1, keepdims=True) + NORM_EPS)
    x_dot_grad = jnp.mean(x_f32 * grad_y, axis=-1, keepdims=True)
    return inv_rms * grad_y - x_f32 * (inv_rms * inv_rms * inv_rms) * x_dot_grad


def block_forward(h_in, gate_w, up_w):
    normed = norm_apply(h_in)
    gate_pre = jnp.dot(normed, gate_w, preferred_element_type=jnp.float32)
    up_pre = jnp.dot(normed, up_w, preferred_element_type=jnp.float32)
    gate_sig = jax.nn.sigmoid(gate_pre)
    gated_act = (gate_pre * gate_sig * up_pre).astype(jnp.bfloat16)
    return normed, gate_pre, up_pre, gate_sig, gated_act


def block_backward(h_in, grad_in, gate_w, up_w, down_w, saved_fwd):
    normed, gate_pre, up_pre, gate_sig, gated_act = saved_fwd
    grad_bf16 = grad_in.astype(jnp.bfloat16)
    grad_act = jnp.dot(grad_bf16, down_w.T, preferred_element_type=jnp.float32)
    grad_gate_pre = (grad_act * up_pre * gate_sig * (1.0 + gate_pre * (1.0 - gate_sig))).astype(jnp.bfloat16)
    grad_up_pre = (grad_act * gate_pre * gate_sig).astype(jnp.bfloat16)
    grad_down_w = jnp.dot(gated_act.T, grad_bf16, preferred_element_type=jnp.float32)
    grad_gate_w = jnp.dot(normed.T, grad_gate_pre, preferred_element_type=jnp.float32)
    grad_up_w = jnp.dot(normed.T, grad_up_pre, preferred_element_type=jnp.float32)
    grad_norm = jnp.dot(grad_gate_pre, gate_w.T, preferred_element_type=jnp.float32) + jnp.dot(grad_up_pre, up_w.T, preferred_element_type=jnp.float32)
    return grad_in + norm_grad(h_in, grad_norm), grad_gate_w, grad_up_w, grad_down_w


def head_grads(h_top, out_w, tgt_ids, mask_ids, mask_count):
    normed_top = norm_apply(h_top)
    logits = jnp.dot(normed_top, out_w, preferred_element_type=jnp.float32)
    shifted = logits - jnp.max(logits, axis=-1, keepdims=True)
    exp_shift = jnp.exp(shifted)
    exp_sum = jnp.sum(exp_shift, axis=-1, keepdims=True)
    is_target = lax.broadcasted_iota(jnp.int32, (1, logits.shape[1]), 1) == tgt_ids[:, None]
    tok_loss = jnp.log(exp_sum[:, 0]) - jnp.sum(jnp.where(is_target, shifted, 0.0), axis=-1)
    weight = mask_ids.astype(jnp.float32) / mask_count
    loss_part = jnp.sum(weight * tok_loss)
    grad_logits = (weight[:, None] * (exp_shift / exp_sum - is_target.astype(jnp.float32))).astype(jnp.bfloat16)
    grad_wout = jnp.dot(normed_top.T, grad_logits, preferred_element_type=jnp.float32)
    grad_top = norm_grad(h_top, jnp.dot(grad_logits, out_w.T, preferred_element_type=jnp.float32))
    return loss_part, grad_wout, grad_top


def reference(hidden, w_gate, w_up, w_down, w_out, targets, loss_mask):
    top_layer = LAYERS - 1
    hidden_blocks = hidden.reshape(LAYERS, GROUP_SIZE, TOK_DEV, HIDDEN)
    mask_count = jnp.sum(loss_mask).astype(jnp.float32)

    def head_step(carry_sums, block_in):
        h_block, tgt_block, mask_block = block_in
        saved_fwd = block_forward(h_block, w_gate[top_layer], w_up[top_layer])
        h_top = (h_block.astype(jnp.float32) + jnp.dot(saved_fwd[4], w_down[top_layer], preferred_element_type=jnp.float32)).astype(jnp.bfloat16)
        loss_part, grad_wout, grad_top = head_grads(h_top, w_out, tgt_block, mask_block, mask_count)
        return (carry_sums[0] + loss_part, carry_sums[1] + grad_wout), grad_top

    head_init = (jnp.zeros((), jnp.float32), jnp.zeros((HIDDEN, VOCAB_SIZE), jnp.float32))
    (mean_loss, grad_out), grad_top = lax.scan(head_step, head_init, (hidden_blocks[top_layer], targets.reshape(GROUP_SIZE, TOK_DEV), loss_mask.reshape(GROUP_SIZE, TOK_DEV)))

    def layer_step(grad_run, layer_in):
        h_layer, gate_w, up_w, down_w = layer_in

        def block_step(carry_sums, block_in):
            h_block, grad_block = block_in
            saved_fwd = block_forward(h_block, gate_w, up_w)
            grad_next, grad_gate_w, grad_up_w, grad_down_w = block_backward(h_block, grad_block, gate_w, up_w, down_w, saved_fwd)
            return (carry_sums[0] + grad_gate_w, carry_sums[1] + grad_up_w, carry_sums[2] + grad_down_w), grad_next

        zero_sums = (jnp.zeros((HIDDEN, FFN_DIM), jnp.float32), jnp.zeros((HIDDEN, FFN_DIM), jnp.float32), jnp.zeros((FFN_DIM, HIDDEN), jnp.float32))
        layer_sums, grad_prev = lax.scan(block_step, zero_sums, (h_layer, grad_run))
        return grad_prev, layer_sums

    grad_first, (grad_gate, grad_up, grad_down) = lax.scan(layer_step, grad_top, (hidden_blocks, w_gate, w_up, w_down), reverse=True)
    grad_hidden = grad_first.reshape(TOKENS, HIDDEN).astype(jnp.bfloat16)
    return grad_gate, grad_up, grad_down, grad_out, grad_hidden, mean_loss
```

```python
import functools

import jax
import jax.numpy as jnp
from jax import lax
from jax.experimental import pallas as pl
from jax.experimental.pallas import tpu as pltpu
from jax.sharding import PartitionSpec as P

EPS = 1e-5
AXIS = 'fsdp'
N_DEV = 16
LAYERS = 5
TOK = 1024
DIM = 576
FFN = 1536
VOCAB = 49152
VLOC = VOCAB // N_DEV
TOKENS = TOK * N_DEV
CHUNKS = 2
TB = TOK // CHUNKS
CHUNK_TOK = TB * N_DEV
ZROWS = TB * 9 // 2
STRIPS = 4
SW = VLOC // STRIPS
PROWS = 1296
BF = jnp.bfloat16
F32 = jnp.float32
VMEM_LIMIT = 62 * 1024 * 1024


def dot_nn(a, b):
    return lax.dot_general(a, b, (((1,), (0,)), ((), ())), preferred_element_type=F32)


def dot_nt(a, b):
    return lax.dot_general(a, b, (((1,), (1,)), ((), ())), preferred_element_type=F32)


def dot_tn(a, b):
    return lax.dot_general(a, b, (((0,), (0,)), ((), ())), preferred_element_type=F32)


def inv_rms_of(x):
    return lax.rsqrt(jnp.mean(x * x, axis=-1, keepdims=True) + EPS)


def norm_grad(x, e):
    r = inv_rms_of(x)
    return r * e - x * (r * r * r) * jnp.mean(x * e, axis=-1, keepdims=True)


def store_packed(ref, val, rows):
    half = rows // 2
    for c in range(4):
        ref[0, c * rows:(c + 1) * rows, :] = val[:, c * 128:(c + 1) * 128]
    ref[0, 4 * rows:4 * rows + half, :] = jnp.concatenate([val[:half, 512:], val[half:, 512:]], axis=1)


def load_packed(dst, ref, rows):
    half = rows // 2
    for c in range(4):
        dst[:, c * 128:(c + 1) * 128] = ref[0, c * rows:(c + 1) * rows, :]
    tail = ref[0, 4 * rows:4 * rows + half, :]
    dst[0:half, 512:576] = tail[:, :64]
    dst[half:rows, 512:576] = tail[:, 64:]


def unpack_rows(p, rows):
    half = rows // 2
    tail = p[4 * rows:]
    tail = jnp.concatenate([tail[:, :64], tail[:, 64:]], axis=0)
    return jnp.concatenate([p[c * rows:(c + 1) * rows] for c in range(4)] + [tail], axis=1)


def fwd_body(h_ref, wg_ref, wu_ref, wd_ref, t_ref, z_ref):
    h = h_ref[...].astype(F32)
    n = (h * inv_rms_of(h)).astype(BF)
    u = dot_nn(n, wg_ref[...])
    v = dot_nn(n, wu_ref[...])
    a = (u * jax.nn.sigmoid(u) * v).astype(BF)
    t = (h + dot_nn(a, wd_ref[...])).astype(BF)
    t_ref[...] = t
    t = t.astype(F32)
    store_packed(z_ref, (t * inv_rms_of(t)).astype(BF), TB)


def top_forward(h, wg, wu, wd):
    full = lambda shape: pl.BlockSpec(shape, lambda i: (0,) * len(shape))
    return pl.pallas_call(
        fwd_body,
        grid=(CHUNKS,),
        in_specs=[pl.BlockSpec((TB, DIM), lambda i: (i, 0)), full((DIM, FFN)), full((DIM, FFN)), full((FFN, DIM))],
        out_specs=[pl.BlockSpec((TB, DIM), lambda i: (i, 0)), pl.BlockSpec((1, ZROWS, 128), lambda i: (i, 0, 0))],
        out_shape=[jax.ShapeDtypeStruct((TOK, DIM), BF), jax.ShapeDtypeStruct((CHUNKS, ZROWS, 128), BF)],
        compiler_params=pltpu.CompilerParams(vmem_limit_bytes=VMEM_LIMIT),
        cost_estimate=pl.CostEstimate(flops=6 * TOK * DIM * FFN, bytes_accessed=10 * 2**20, transcendentals=TOK * FFN),
        name='top_forward',
    )(h, wg, wu, wd)


def pass1_body(z_ref, w_ref, tok_ref, e_ref, ms_ref, st_ref, z_s):
    load_packed(z_s, z_ref, TB)
    z = z_s[...]
    tokc = jnp.concatenate([tok_ref[...], jnp.zeros((120, TB), F32)], axis=0).T
    tgt = tokc[:, 0:1]
    lane = lax.broadcasted_iota(jnp.int32, (TB, 128), 1)
    ids = lax.broadcasted_iota(jnp.int32, (1, SW), 1).astype(F32)
    ms = jnp.zeros((TB, 128), F32)
    tl = jnp.zeros((TB, 1), F32)
    m_list, s_list = [], []
    for s in range(STRIPS):
        l = dot_nn(z, w_ref[:, s * SW:(s + 1) * SW])
        m = jnp.max(l, axis=1, keepdims=True)
        e = jnp.exp(l - m)
        e_ref[:, s * SW:(s + 1) * SW] = e
        s_list.append(jnp.sum(e, axis=1, keepdims=True))
        m_list.append(m)
        tl = tl + jnp.sum(jnp.where(ids == tgt - float(s * SW), l, 0.0), axis=1, keepdims=True)
        ms = jnp.where(lane == s, m, ms)
    m_all = functools.reduce(jnp.maximum, m_list)
    s_all = sum(sv * jnp.exp(mv - m_all) for sv, mv in zip(s_list, m_list))
    ms_ref[...] = ms
    st = jnp.where(lane == 0, m_all, jnp.where(lane == 1, s_all, jnp.where(lane == 2, tl, 0.0)))
    st_ref[...] = st.T[0:8, :]


def head_pass1(z_all, w, tok):
    return pl.pallas_call(
        pass1_body,
        grid=(N_DEV,),
        in_specs=[
            pl.BlockSpec((1, ZROWS, 128), lambda i: (i, 0, 0)),
            pl.BlockSpec((DIM, VLOC), lambda i: (0, 0)),
            pl.BlockSpec((8, TB), lambda i: (0, i)),
        ],
        out_specs=[
            pl.BlockSpec((TB, VLOC), lambda i: (i, 0)),
            pl.BlockSpec((TB, 128), lambda i: (i, 0)),
            pl.BlockSpec((8, TB), lambda i: (0, i)),
        ],
        out_shape=[
            jax.ShapeDtypeStruct((CHUNK_TOK, VLOC), F32),
            jax.ShapeDtypeStruct((CHUNK_TOK, 128), F32),
            jax.ShapeDtypeStruct((8, CHUNK_TOK), F32),
        ],
        scratch_shapes=[pltpu.VMEM((TB, DIM), BF)],
        compiler_params=pltpu.CompilerParams(vmem_limit_bytes=VMEM_LIMIT),
        cost_estimate=pl.CostEstimate(flops=2 * CHUNK_TOK * DIM * VLOC, bytes_accessed=4 * CHUNK_TOK * VLOC, transcendentals=CHUNK_TOK * VLOC),
        name='head_pass1',
    )(z_all, w, tok)


def pass2_body(has_acc, *refs):
    if has_acc:
        z_ref, w_ref, tok_ref, e_ref, ms_ref, acc_ref, dz_ref, gw_ref, z_s, q_s = refs
    else:
        z_ref, w_ref, tok_ref, e_ref, ms_ref, dz_ref, gw_ref, z_s, q_s = refs
        acc_ref = None

    @pl.when(pl.program_id(0) == 0)
    def _():
        if has_acc:
            gw_ref[...] = acc_ref[...]
        else:
            gw_ref[...] = jnp.zeros_like(gw_ref)

    load_packed(z_s, z_ref, TB)
    z = z_s[...]
    tokc = jnp.concatenate([tok_ref[...], jnp.zeros((120, TB), F32)], axis=0).T
    tgt, w_tok, m_glob, s_inv = (tokc[:, i:i + 1] for i in range(4))
    ids = lax.broadcasted_iota(jnp.int32, (1, SW), 1).astype(F32)
    for s in range(STRIPS):
        cols = slice(s * SW, (s + 1) * SW)
        scale = jnp.exp(ms_ref[:, s:s + 1] - m_glob) * s_inv
        p = e_ref[:, cols] * scale
        p = jnp.where(ids == tgt - float(s * SW), p - 1.0, p)
        q = (w_tok * p).astype(BF)
        q_s[:, cols] = q
        gw_ref[:, cols] += dot_tn(z, q)
    dz = dot_nt(q_s[...], w_ref[...])
    store_packed(dz_ref, dz, TB)


def head_pass2(z_all, w, tok, e, ms, acc):
    in_specs = [
        pl.BlockSpec((1, ZROWS, 128), lambda i: (i, 0, 0)),
        pl.BlockSpec((DIM, VLOC), lambda i: (0, 0)),
        pl.BlockSpec((8, TB), lambda i: (0, i)),
        pl.BlockSpec((TB, VLOC), lambda i: (i, 0)),
        pl.BlockSpec((TB, 128), lambda i: (i, 0)),
    ]
    args = [z_all, w, tok, e, ms]
    if acc is not None:
        in_specs.append(pl.BlockSpec((DIM, VLOC), lambda i: (0, 0), pipeline_mode=pl.Buffered(1)))
        args.append(acc)
    return pl.pallas_call(
        functools.partial(pass2_body, acc is not None),
        grid=(N_DEV,),
        in_specs=in_specs,
        out_specs=[
            pl.BlockSpec((1, ZROWS, 128), lambda i: (i, 0, 0)),
            pl.BlockSpec((DIM, VLOC), lambda i: (0, 0), pipeline_mode=pl.Buffered(1)),
        ],
        out_shape=[
            jax.ShapeDtypeStruct((N_DEV, ZROWS, 128), F32),
            jax.ShapeDtypeStruct((DIM, VLOC), F32),
        ],
        scratch_shapes=[pltpu.VMEM((TB, DIM), BF), pltpu.VMEM((TB, VLOC), BF)],
        compiler_params=pltpu.CompilerParams(vmem_limit_bytes=VMEM_LIMIT),
        cost_estimate=pl.CostEstimate(flops=4 * CHUNK_TOK * DIM * VLOC, bytes_accessed=4 * CHUNK_TOK * VLOC, transcendentals=0),
        name='head_pass2',
    )(*args)


BT = 256


def bwd_body(off, has_buf, *refs):
    if has_buf:
        h_ref, g_ref, wg_ref, wu_ref, wd_ref, _, go_ref, buf_ref, n_s, k_s, a_s, du_s, dv_s, pk_s, sem = refs
    else:
        h_ref, g_ref, wg_ref, wu_ref, wd_ref, go_ref, buf_ref, n_s, k_s, a_s, du_s, dv_s, pk_s, sem = refs

    def step(i, carry):
        rows = pl.ds(pl.multiple_of(i * BT, BT), BT)
        h = h_ref[rows, :].astype(F32)
        r = inv_rms_of(h)
        n = (h * r).astype(BF)
        g = g_ref[rows, :]
        k = g.astype(BF)
        u = dot_nn(n, wg_ref[...])
        v = dot_nn(n, wu_ref[...])
        e = dot_nt(k, wd_ref[...])
        sg = jax.nn.sigmoid(u)
        us = u * sg
        a = (us * v).astype(BF)
        du = (e * v * sg * (1.0 + u * (1.0 - sg))).astype(BF)
        dv = (e * us).astype(BF)
        n_s[rows, :] = n
        k_s[rows, :] = k
        a_s[rows, :] = a
        du_s[rows, :] = du
        dv_s[rows, :] = dv
        dn = dot_nt(du, wg_ref[...]) + dot_nt(dv, wu_ref[...])
        go_ref[rows, :] = (g + r * dn - h * (r * r * r) * jnp.mean(h * dn, axis=-1, keepdims=True)).astype(go_ref.dtype)
        return carry

    lax.fori_loop(0, TOK // BT, step, 0)
    n = n_s[...]
    k = k_s[...]
    for c in range(6):
        gg = dot_tn(n, du_s[:, c * 256:(c + 1) * 256])
        gu = dot_tn(n, dv_s[:, c * 256:(c + 1) * 256])
        for j in range(2):
            base = (2 * c + j) * 72
            for d in range(N_DEV):
                pk_s[d, base:base + 36, :] = gg[36 * d:36 * d + 36, j * 128:(j + 1) * 128]
                pk_s[d, base + 36:base + 72, :] = gu[36 * d:36 * d + 36, j * 128:(j + 1) * 128]
    for c in range(4):
        gd = dot_tn(a_s[:, c * 384:(c + 1) * 384], k)
        for j in range(4):
            d = c * 4 + j
            x = gd[96 * j:96 * j + 96, :]
            for b in range(4):
                pk_s[d, 864 + 96 * b:864 + 96 * b + 96, :] = x[:, 128 * b:128 * b + 128]
            pk_s[d, 1248:1296, :] = jnp.concatenate([x[:48, 512:], x[48:, 512:]], axis=1)
    copy = pltpu.make_async_copy(pk_s, buf_ref.at[:, pl.ds(off, PROWS), :], sem)
    copy.start()
    copy.wait()


def block_backward(h, g, wg, wu, wd, buf, slot, slots, out_dtype):
    vm = pl.BlockSpec(memory_space=pltpu.VMEM)
    hb = pl.BlockSpec(memory_space=pl.ANY)
    args = [h, g, wg, wu, wd]
    in_specs = [vm] * 5
    aliases = {}
    if buf is not None:
        args.append(buf)
        in_specs.append(hb)
        aliases = {5: 1}
    return pl.pallas_call(
        functools.partial(bwd_body, slot * PROWS, buf is not None),
        in_specs=in_specs,
        out_specs=[vm, hb],
        out_shape=[jax.ShapeDtypeStruct((TOK, DIM), out_dtype), jax.ShapeDtypeStruct((N_DEV, slots * PROWS, 128), F32)],
        scratch_shapes=[
            pltpu.VMEM((TOK, DIM), BF), pltpu.VMEM((TOK, DIM), BF), pltpu.VMEM((TOK, FFN), BF),
            pltpu.VMEM((TOK, FFN), BF), pltpu.VMEM((TOK, FFN), BF), pltpu.VMEM((N_DEV, PROWS, 128), F32),
            pltpu.SemaphoreType.DMA,
        ],
        input_output_aliases=aliases,
        compiler_params=pltpu.CompilerParams(vmem_limit_bytes=VMEM_LIMIT),
        cost_estimate=pl.CostEstimate(flops=16 * TOK * DIM * FFN, bytes_accessed=24 * 2**20, transcendentals=TOK * FFN),
        name='block_backward',
    )(*args)


def unpack_body(p_ref, gg_ref, gu_ref, gd_ref):
    for c in range(12):
        gg_ref[0, :, c * 128:(c + 1) * 128] = p_ref[c * 72:c * 72 + 36, :]
        gu_ref[0, :, c * 128:(c + 1) * 128] = p_ref[c * 72 + 36:c * 72 + 72, :]
    for b in range(4):
        gd_ref[0, :, b * 128:(b + 1) * 128] = p_ref[864 + 96 * b:864 + 96 * b + 96, :]
    tail = p_ref[1248:1296, :]
    gd_ref[0, 0:48, 512:576] = tail[:, :64]
    gd_ref[0, 48:96, 512:576] = tail[:, 64:]


def unpack_grads(packed):
    return pl.pallas_call(
        unpack_body,
        grid=(LAYERS,),
        in_specs=[pl.BlockSpec((PROWS, 128), lambda i: (i, 0))],
        out_specs=[
            pl.BlockSpec((1, 36, FFN), lambda i: (i, 0, 0)),
            pl.BlockSpec((1, 36, FFN), lambda i: (i, 0, 0)),
            pl.BlockSpec((1, 96, DIM), lambda i: (i, 0, 0)),
        ],
        out_shape=[
            jax.ShapeDtypeStruct((LAYERS, 36, FFN), F32),
            jax.ShapeDtypeStruct((LAYERS, 36, FFN), F32),
            jax.ShapeDtypeStruct((LAYERS, 96, DIM), F32),
        ],
        name='unpack_grads',
    )(packed)


def pack_weights(wg, wu, wd):
    tail = jnp.concatenate([wd[:48, 512:], wd[48:, 512:]], axis=1)
    return jnp.concatenate(
        [wg.reshape(432, 128), wu.reshape(432, 128)] + [wd[:, c * 128:(c + 1) * 128] for c in range(4)] + [tail], axis=0)


def unpack_weights(p):
    wg = p[:, :432].reshape(DIM, FFN)
    wu = p[:, 432:864].reshape(DIM, FFN)
    tail = p[:, 1248:]
    tail = jnp.concatenate([tail[:, :, :64], tail[:, :, 64:]], axis=1)
    wd = jnp.concatenate([p[:, 864 + 96 * c:864 + 96 * c + 96] for c in range(4)] + [tail], axis=2)
    return wg, wu, wd.reshape(FFN, DIM)


GROUPS = ((4, 3), (2, 1, 0))


def solution(mesh):
    def device_step(hidden, w_gate, w_up, w_down, w_out, targets, loss_mask):
        me = lax.axis_index(AXIS)
        gather = functools.partial(lax.all_gather, axis_name=AXIS)
        packs = [pack_weights(w_gate[l], w_up[l], w_down[l]) for l in range(LAYERS)]
        weights = [None] * LAYERS
        weights[4] = unpack_weights(gather(packs[4]))
        lab = gather(jnp.stack([targets, loss_mask]))
        w_vocab = lax.all_to_all(w_out.reshape(36, N_DEV, VLOC), AXIS, 1, 0).reshape(DIM, VLOC)
        t, z_packed = top_forward(hidden[4], *weights[4])

        mask = lab[:, 1, :].astype(F32)
        w_tok = mask / jnp.sum(mask)
        tgt = (lab[:, 0, :] - me * VLOC).astype(F32)

        z_all, rest = [], None
        for c in range(CHUNKS):
            z_all.append(gather(z_packed[c]))
        rest = gather(jnp.stack(packs[:4]))
        acc, loss, g_rows = None, jnp.zeros((), F32), []
        for c in range(CHUNKS):
            sl = slice(c * TB, (c + 1) * TB)
            tg = tgt[:, sl].reshape(1, CHUNK_TOK)
            wt = w_tok[:, sl].reshape(1, CHUNK_TOK)
            zero = jnp.zeros((1, CHUNK_TOK), F32)
            e, ms, st = head_pass1(z_all[c], w_vocab, jnp.concatenate([tg] + [zero] * 7, axis=0))
            m_glob = lax.pmax(st[0:1], AXIS)
            sums = lax.psum(jnp.concatenate([st[1:2] * jnp.exp(st[0:1] - m_glob), st[2:3]], axis=0), AXIS)
            loss = loss + jnp.sum(wt * (m_glob + jnp.log(sums[0:1]) - sums[1:2]))
            tok = jnp.concatenate([tg, wt, m_glob, 1.0 / sums[0:1]] + [zero] * 4, axis=0)
            dz, acc = head_pass2(z_all[c], w_vocab, tok, e, ms, acc)
            dz = lax.psum_scatter(dz, AXIS, scatter_dimension=0, tiled=False)
            g_rows.append(norm_grad(t[sl].astype(F32), unpack_rows(dz, TB)))
        grad_out = lax.all_to_all(acc.reshape(N_DEV, 36, VLOC), AXIS, 0, 1)
        grad_out = grad_out.reshape(36, VOCAB)
        for l in range(4):
            weights[l] = unpack_weights(rest[:, l])

        g = jnp.concatenate(g_rows, axis=0)
        packed = [None] * LAYERS
        for group in GROUPS:
            buf = None
            for i, l in enumerate(group):
                g, buf = block_backward(hidden[l], g, *weights[l], buf, i, len(group), BF if l == 0 else F32)
            red = lax.psum_scatter(buf, AXIS, scatter_dimension=0, tiled=False)
            for i, l in enumerate(group):
                packed[l] = red[i * PROWS:(i + 1) * PROWS]
        grad_gate, grad_up, grad_down = unpack_grads(jnp.concatenate(packed, axis=0))
        return grad_gate, grad_up, grad_down, grad_out, g, loss

    stacked = P(None, AXIS, None)
    row = P(AXIS, None)
    return jax.shard_map(device_step, mesh=mesh, in_specs=(stacked, stacked, stacked, stacked, row, P(AXIS), P(AXIS)), out_specs=(stacked, stacked, stacked, row, row, P()), check_vma=False)
```

```python
import functools

import jax
import jax.numpy as jnp
from jax import lax
from jax.experimental import pallas as pl
from jax.experimental.pallas import tpu as pltpu
from jax.sharding import PartitionSpec as P

EPS = 1e-5
AXIS = 'fsdp'
N_DEV = 16
LAYERS = 5
TOK = 1024
DIM = 576
FFN = 1536
VOCAB = 49152
VLOC = VOCAB // N_DEV
TOKENS = TOK * N_DEV
CHUNKS = 2
TB = TOK // CHUNKS
CHUNK_TOK = TB * N_DEV
ZROWS = TB * 9 // 2
STRIPS = 4
SW = VLOC // STRIPS
PROWS = 1296
BF = jnp.bfloat16
F32 = jnp.float32
MESH = pl.DeviceIdType.MESH
VMEM_LIMIT = 62 * 1024 * 1024


def whole(*shape):
    return pl.BlockSpec(shape, lambda i: tuple(0 * d for d in shape))


def rows_spec(*shape):
    rest = shape[1:]
    return pl.BlockSpec(shape, lambda i: (i, *(0 * d for d in rest)))


def lanes_spec(*shape):
    return pl.BlockSpec(shape, lambda i: (0, i))


VM = pl.BlockSpec(memory_space=pltpu.VMEM)
HB = pl.BlockSpec(memory_space=pl.ANY)


def dot_nn(a, b):
    return lax.dot_general(a, b, (((1,), (0,)), ((), ())), preferred_element_type=F32)


def dot_nt(a, b):
    return lax.dot_general(a, b, (((1,), (1,)), ((), ())), preferred_element_type=F32)


def dot_tn(a, b):
    return lax.dot_general(a, b, (((0,), (0,)), ((), ())), preferred_element_type=F32)


def inv_rms_of(x):
    return lax.rsqrt(jnp.mean(x * x, axis=-1, keepdims=True) + EPS)


def norm_grad(x, e):
    r = inv_rms_of(x)
    return r * e - x * (r * r * r) * jnp.mean(x * e, axis=-1, keepdims=True)


def store_packed(ref, val, rows):
    half = rows // 2
    for c in range(4):
        ref[0, c * rows:(c + 1) * rows, :] = val[:, c * 128:(c + 1) * 128]
    ref[0, 4 * rows:4 * rows + half, :] = jnp.concatenate([val[:half, 512:], val[half:, 512:]], axis=1)


def load_packed(dst, ref, rows):
    half = rows // 2
    for c in range(4):
        dst[:, c * 128:(c + 1) * 128] = ref[0, c * rows:(c + 1) * rows, :]
    tail = ref[0, 4 * rows:4 * rows + half, :]
    dst[0:half, 512:576] = tail[:, :64]
    dst[half:rows, 512:576] = tail[:, 64:]


def unpack_rows(p, rows):
    half = rows // 2
    tail = p[4 * rows:]
    tail = jnp.concatenate([tail[:, :64], tail[:, 64:]], axis=0)
    return jnp.concatenate([p[c * rows:(c + 1) * rows] for c in range(4)] + [tail], axis=1)


W_SCRATCH = [pltpu.VMEM((DIM, FFN), BF), pltpu.VMEM((DIM, FFN), BF), pltpu.VMEM((FFN, DIM), BF)]


def fwd_body(h_ref, p_ref, t_ref, z_ref, wg_ref, wu_ref, wd_ref):
    @pl.when(pl.program_id(0) == 0)
    def _():
        unpack_weights(p_ref, 0, wg_ref, wu_ref, wd_ref)

    h = h_ref[...].astype(F32)
    n = (h * inv_rms_of(h)).astype(BF)
    u = dot_nn(n, wg_ref[...])
    v = dot_nn(n, wu_ref[...])
    a = (u * jax.nn.sigmoid(u) * v).astype(BF)
    t = (h + dot_nn(a, wd_ref[...])).astype(BF)
    t_ref[...] = t
    t = t.astype(F32)
    store_packed(z_ref, (t * inv_rms_of(t)).astype(BF), TB)


def top_forward(h, packs):
    return pl.pallas_call(
        fwd_body,
        grid=(CHUNKS,),
        in_specs=[rows_spec(TB, DIM), whole(N_DEV, 1, PROWS, 128)],
        out_specs=[rows_spec(TB, DIM), rows_spec(1, ZROWS, 128)],
        out_shape=[jax.ShapeDtypeStruct((TOK, DIM), BF), jax.ShapeDtypeStruct((CHUNKS, ZROWS, 128), BF)],
        scratch_shapes=W_SCRATCH,
        compiler_params=pltpu.CompilerParams(vmem_limit_bytes=VMEM_LIMIT),
        cost_estimate=pl.CostEstimate(flops=6 * TOK * DIM * FFN, bytes_accessed=10 * 2**20, transcendentals=TOK * FFN),
        name='top_forward',
    )(h, packs)


def peers_barrier(me):
    sem = pltpu.get_barrier_semaphore()
    for off in range(1, N_DEV):
        pl.semaphore_signal(sem, inc=1, device_id=(lax.rem(me + off, N_DEV),), device_id_type=MESH)
    pl.semaphore_wait(sem, N_DEV - 1)


def all_send(me, src_of, dst, send_sem, recv_sem):
    copies = []
    for off in range(1, N_DEV):
        to = lax.rem(me + off, N_DEV)
        copy = pltpu.make_async_remote_copy(
            src_ref=src_of(to), dst_ref=dst.at[me], send_sem=send_sem.at[off], recv_sem=recv_sem.at[me],
            device_id=(to,), device_id_type=MESH)
        copy.start()
        copies.append(copy)
    return copies


def all_wait(me, src_of, dst, send_sem, recv_sem):
    for off in range(1, N_DEV):
        frm = lax.rem(me + N_DEV - off, N_DEV)
        copy = pltpu.make_async_remote_copy(
            src_ref=src_of(frm), dst_ref=dst.at[frm], send_sem=send_sem.at[off], recv_sem=recv_sem.at[frm],
            device_id=(frm,), device_id_type=MESH)
        copy.wait_recv()


def labels_body(x_ref, o_ref, buf, send_sem, recv_sem):
    me = lax.axis_index(AXIS)
    peers_barrier(me)
    src = lambda j: x_ref
    copies = all_send(me, src, buf, send_sem, recv_sem)
    all_wait(me, src, buf, send_sem, recv_sem)
    for copy in copies:
        copy.wait_send()
    for j in range(N_DEV):
        o_ref[j] = jnp.where(me == j, x_ref[...], buf[j])


def gather_labels(x):
    return pl.pallas_call(
        labels_body,
        in_specs=[VM],
        out_specs=VM,
        out_shape=jax.ShapeDtypeStruct((N_DEV, 8, TOK), F32),
        scratch_shapes=[pltpu.VMEM((N_DEV, 8, TOK), F32), pltpu.SemaphoreType.DMA((N_DEV,)), pltpu.SemaphoreType.DMA((N_DEV,))],
        compiler_params=pltpu.CompilerParams(collective_id=1, has_side_effects=True),
        cost_estimate=pl.CostEstimate(flops=2 * 10**9, bytes_accessed=2**20, transcendentals=0),
        name='gather_labels',
    )(x)


def stats_body(st_ref, w_ref, o_ref, buf1, own, buf2, send1, recv1, send2, recv2):
    me = lax.axis_index(AXIS)
    peers_barrier(me)
    part = lambda j: st_ref.at[:, pl.ds(pl.multiple_of(j * TB, TB), TB)]
    copies = all_send(me, part, buf1, send1, recv1)
    all_wait(me, part, buf1, send1, recv1)
    mine = st_ref[:, pl.ds(pl.multiple_of(me * TB, TB), TB)]
    rows = [jnp.where(me == j, mine, buf1[j]) for j in range(N_DEV)]
    m = functools.reduce(jnp.maximum, [r[0:1] for r in rows])
    s = sum(r[1:2] * jnp.exp(r[0:1] - m) for r in rows)
    t = sum(r[2:3] for r in rows)
    own[...] = jnp.concatenate([m, 1.0 / s, w_ref[0:1, :] * (m + jnp.log(s) - t), jnp.zeros((5, TB), F32)], axis=0)
    src = lambda j: own
    copies += all_send(me, src, buf2, send2, recv2)
    all_wait(me, src, buf2, send2, recv2)
    for copy in copies:
        copy.wait_send()
    for j in range(N_DEV):
        o_ref[:, j * TB:(j + 1) * TB] = jnp.where(me == j, own[...], buf2[j])


def exchange_stats(st, w_own, cid):
    return pl.pallas_call(
        stats_body,
        in_specs=[VM, VM],
        out_specs=VM,
        out_shape=jax.ShapeDtypeStruct((8, CHUNK_TOK), F32),
        scratch_shapes=[
            pltpu.VMEM((N_DEV, 8, TB), F32), pltpu.VMEM((8, TB), F32), pltpu.VMEM((N_DEV, 8, TB), F32),
            pltpu.SemaphoreType.DMA((N_DEV,)), pltpu.SemaphoreType.DMA((N_DEV,)),
            pltpu.SemaphoreType.DMA((N_DEV,)), pltpu.SemaphoreType.DMA((N_DEV,)),
        ],
        compiler_params=pltpu.CompilerParams(collective_id=cid, has_side_effects=True),
        cost_estimate=pl.CostEstimate(flops=2 * 10**9, bytes_accessed=2**20, transcendentals=0),
        name='exchange_stats',
    )(st, w_own)


def pass1_body(z_ref, w_ref, tok_ref, e_ref, ms_ref, st_ref, z_s):
    load_packed(z_s, z_ref, TB)
    z = z_s[...]
    tokc = jnp.concatenate([tok_ref[...], jnp.zeros((120, TB), F32)], axis=0).T
    tgt = tokc[:, 0:1]
    lane = lax.broadcasted_iota(jnp.int32, (TB, 128), 1)
    ids = lax.broadcasted_iota(jnp.int32, (1, SW), 1).astype(F32)
    ms = jnp.zeros((TB, 128), F32)
    tl = jnp.zeros((TB, 1), F32)
    m_list, s_list = [], []
    for s in range(STRIPS):
        l = dot_nn(z, w_ref[:, s * SW:(s + 1) * SW])
        m = jnp.max(l, axis=1, keepdims=True)
        e = jnp.exp(l - m)
        e_ref[:, s * SW:(s + 1) * SW] = e
        s_list.append(jnp.sum(e, axis=1, keepdims=True))
        m_list.append(m)
        tl = tl + jnp.sum(jnp.where(ids == tgt - float(s * SW), l, 0.0), axis=1, keepdims=True)
        ms = jnp.where(lane == s, m, ms)
    m_all = functools.reduce(jnp.maximum, m_list)
    s_all = sum(sv * jnp.exp(mv - m_all) for sv, mv in zip(s_list, m_list))
    ms_ref[...] = ms
    st = jnp.where(lane == 0, m_all, jnp.where(lane == 1, s_all, jnp.where(lane == 2, tl, 0.0)))
    st_ref[...] = st.T[0:8, :]


def head_pass1(z_all, w, tok):
    return pl.pallas_call(
        pass1_body,
        grid=(N_DEV,),
        in_specs=[
            rows_spec(1, ZROWS, 128),
            whole(DIM, VLOC),
            lanes_spec(8, TB),
        ],
        out_specs=[
            rows_spec(TB, VLOC),
            rows_spec(TB, 128),
            lanes_spec(8, TB),
        ],
        out_shape=[
            jax.ShapeDtypeStruct((CHUNK_TOK, VLOC), F32),
            jax.ShapeDtypeStruct((CHUNK_TOK, 128), F32),
            jax.ShapeDtypeStruct((8, CHUNK_TOK), F32),
        ],
        scratch_shapes=[pltpu.VMEM((TB, DIM), BF)],
        compiler_params=pltpu.CompilerParams(vmem_limit_bytes=VMEM_LIMIT),
        cost_estimate=pl.CostEstimate(flops=2 * CHUNK_TOK * DIM * VLOC, bytes_accessed=4 * CHUNK_TOK * VLOC, transcendentals=CHUNK_TOK * VLOC),
        name='head_pass1',
    )(z_all, w, tok)


def pass2_body(has_acc, *refs):
    if has_acc:
        z_ref, w_ref, tok_ref, res_ref, e_ref, ms_ref, acc_ref, dz_ref, gw_ref, z_s, q_s = refs
    else:
        z_ref, w_ref, tok_ref, res_ref, e_ref, ms_ref, dz_ref, gw_ref, z_s, q_s = refs
        acc_ref = None

    @pl.when(pl.program_id(0) == 0)
    def _():
        if has_acc:
            gw_ref[...] = acc_ref[...]
        else:
            gw_ref[...] = jnp.zeros_like(gw_ref)

    load_packed(z_s, z_ref, TB)
    z = z_s[...]
    tokc = jnp.concatenate([tok_ref[...], res_ref[...], jnp.zeros((112, TB), F32)], axis=0).T
    tgt, w_tok, m_glob, s_inv = (tokc[:, i:i + 1] for i in (0, 1, 8, 9))
    ids = lax.broadcasted_iota(jnp.int32, (1, SW), 1).astype(F32)
    for s in range(STRIPS):
        cols = slice(s * SW, (s + 1) * SW)
        scale = jnp.exp(ms_ref[:, s:s + 1] - m_glob) * s_inv
        p = e_ref[:, cols] * scale
        p = jnp.where(ids == tgt - float(s * SW), p - 1.0, p)
        q = (w_tok * p).astype(BF)
        q_s[:, cols] = q
        gw_ref[:, cols] += dot_tn(z, q)
    dz = dot_nt(q_s[...], w_ref[...])
    store_packed(dz_ref, dz, TB)


def head_pass2(z_all, w, tok, res, e, ms, acc):
    in_specs = [
        rows_spec(1, ZROWS, 128),
        whole(DIM, VLOC),
        lanes_spec(8, TB),
        lanes_spec(8, TB),
        rows_spec(TB, VLOC),
        rows_spec(TB, 128),
    ]
    args = [z_all, w, tok, res, e, ms]
    if acc is not None:
        in_specs.append(pl.BlockSpec((DIM, VLOC), lambda i: (0, 0), pipeline_mode=pl.Buffered(1)))
        args.append(acc)
    return pl.pallas_call(
        functools.partial(pass2_body, acc is not None),
        grid=(N_DEV,),
        in_specs=in_specs,
        out_specs=[
            rows_spec(1, ZROWS, 128),
            pl.BlockSpec((DIM, VLOC), lambda i: (0, 0), pipeline_mode=pl.Buffered(1)),
        ],
        out_shape=[
            jax.ShapeDtypeStruct((N_DEV, ZROWS, 128), F32),
            jax.ShapeDtypeStruct((DIM, VLOC), F32),
        ],
        scratch_shapes=[pltpu.VMEM((TB, DIM), BF), pltpu.VMEM((TB, VLOC), BF)],
        compiler_params=pltpu.CompilerParams(vmem_limit_bytes=VMEM_LIMIT),
        cost_estimate=pl.CostEstimate(flops=4 * CHUNK_TOK * DIM * VLOC, bytes_accessed=4 * CHUNK_TOK * VLOC, transcendentals=0),
        name='head_pass2',
    )(*args)


BT = 512


def bwd_body(top, off, *refs):
    if top:
        h_ref, p_ref, t_ref, d0_ref, d1_ref, go_ref, buf_ref, *scratch = refs
    else:
        h_ref, p_ref, g_ref, buf_in, go_ref, buf_ref, *scratch = refs
    _, wg_ref, wu_ref, wd_ref, n_s, k_s, a_s, du_s, dv_s, pk_s, sem = scratch
    unpack_weights(p_ref, 0, wg_ref, wu_ref, wd_ref)

    for i in range(TOK // BT):
        rows = slice(i * BT, (i + 1) * BT)
        h = h_ref[rows, :].astype(F32)
        r = inv_rms_of(h)
        n = (h * r).astype(BF)
        if top:
            g = norm_grad(t_ref[rows, :].astype(F32), unpack_rows((d0_ref, d1_ref)[i], TB))
        else:
            g = g_ref[rows, :]
        k = g.astype(BF)
        u = dot_nn(n, wg_ref[...])
        v = dot_nn(n, wu_ref[...])
        e = dot_nt(k, wd_ref[...])
        sg = jax.nn.sigmoid(u)
        us = u * sg
        a_s[rows, :] = (us * v).astype(BF)
        du = (e * v * sg * (1.0 + u * (1.0 - sg))).astype(BF)
        dv = (e * us).astype(BF)
        n_s[rows, :] = n
        k_s[rows, :] = k
        du_s[rows, :] = du
        dv_s[rows, :] = dv
        dn = dot_nt(du, wg_ref[...]) + dot_nt(dv, wu_ref[...])
        go_ref[rows, :] = (g + r * dn - h * (r * r * r) * jnp.mean(h * dn, axis=-1, keepdims=True)).astype(go_ref.dtype)

    n = n_s[...]
    k = k_s[...]
    for c in range(6):
        gg = dot_tn(n, du_s[:, c * 256:(c + 1) * 256])
        gu = dot_tn(n, dv_s[:, c * 256:(c + 1) * 256])
        for j in range(2):
            base = (2 * c + j) * 72
            for d in range(N_DEV):
                pk_s[d, base:base + 36, :] = gg[36 * d:36 * d + 36, j * 128:(j + 1) * 128]
                pk_s[d, base + 36:base + 72, :] = gu[36 * d:36 * d + 36, j * 128:(j + 1) * 128]
    copy_a = pltpu.make_async_copy(pk_s.at[:, pl.ds(0, 864), :], buf_ref.at[:, pl.ds(off, 864), :], sem.at[0])
    copy_a.start()
    for c in range(4):
        gd = dot_tn(a_s[:, c * 384:(c + 1) * 384], k)
        for j in range(4):
            d = c * 4 + j
            x = gd[96 * j:96 * j + 96, :]
            for b in range(4):
                pk_s[d, 864 + 96 * b:864 + 96 * b + 96, :] = x[:, 128 * b:128 * b + 128]
            pk_s[d, 1248:1296, :] = jnp.concatenate([x[:48, 512:], x[48:, 512:]], axis=1)
    copy_b = pltpu.make_async_copy(pk_s.at[:, pl.ds(864, 432), :], buf_ref.at[:, pl.ds(off + 864, 432), :], sem.at[1])
    copy_b.start()
    copy_a.wait()
    copy_b.wait()


def block_backward(h, packs, wslot, g_args, buf, slot, slots, out_dtype):
    top = len(g_args) == 3
    args = [h, packs, *g_args]
    in_specs = [whole(TOK, DIM), pl.BlockSpec((N_DEV, 1, PROWS, 128), lambda i: (0, wslot, 0, 0))]
    in_specs += [whole(*x.shape) for x in g_args]
    aliases = {}
    if not top:
        args.append(jnp.zeros((8, 128), F32) if buf is None else buf)
        in_specs.append(HB)
        aliases = {} if buf is None else {3: 1}
    return pl.pallas_call(
        functools.partial(bwd_body, top, slot * PROWS),
        grid=(1,),
        in_specs=in_specs,
        out_specs=[whole(TOK, DIM), HB],
        out_shape=[jax.ShapeDtypeStruct((TOK, DIM), out_dtype), jax.ShapeDtypeStruct((N_DEV, slots * PROWS, 128), F32)],
        scratch_shapes=[pltpu.SMEM((1,), jnp.int32)] + W_SCRATCH + [
            pltpu.VMEM((TOK, DIM), BF), pltpu.VMEM((TOK, DIM), BF), pltpu.VMEM((TOK, FFN), BF),
            pltpu.VMEM((TOK, FFN), BF), pltpu.VMEM((TOK, FFN), BF), pltpu.VMEM((N_DEV, PROWS, 128), F32),
            pltpu.SemaphoreType.DMA((2,)),
        ],
        input_output_aliases=aliases,
        compiler_params=pltpu.CompilerParams(vmem_limit_bytes=VMEM_LIMIT),
        cost_estimate=pl.CostEstimate(flops=16 * TOK * DIM * FFN, bytes_accessed=24 * 2**20, transcendentals=TOK * FFN),
        name='block_backward',
    )(*args)


def unpack_body(has_prev, p_ref, *refs):
    gg_ref, gu_ref, gd_ref = refs[3:] if has_prev else refs
    for c in range(12):
        gg_ref[0, :, c * 128:(c + 1) * 128] = p_ref[c * 72:c * 72 + 36, :]
        gu_ref[0, :, c * 128:(c + 1) * 128] = p_ref[c * 72 + 36:c * 72 + 72, :]
    for b in range(4):
        gd_ref[0, :, b * 128:(b + 1) * 128] = p_ref[864 + 96 * b:864 + 96 * b + 96, :]
    tail = p_ref[1248:1296, :]
    gd_ref[0, 0:48, 512:576] = tail[:, :64]
    gd_ref[0, 48:96, 512:576] = tail[:, 64:]


def unpack_grads(packed, group, prev):
    prev = list(prev or ())
    back = lambda i: (group[0] - i, 0, 0)
    return pl.pallas_call(
        functools.partial(unpack_body, bool(prev)),
        grid=(len(group),),
        in_specs=[rows_spec(PROWS, 128)] + [HB] * len(prev),
        out_specs=[
            pl.BlockSpec((1, 36, FFN), back),
            pl.BlockSpec((1, 36, FFN), back),
            pl.BlockSpec((1, 96, DIM), back),
        ],
        out_shape=[
            jax.ShapeDtypeStruct((LAYERS, 36, FFN), F32),
            jax.ShapeDtypeStruct((LAYERS, 36, FFN), F32),
            jax.ShapeDtypeStruct((LAYERS, 96, DIM), F32),
        ],
        input_output_aliases={1 + i: i for i in range(len(prev))},
        name='unpack_grads',
    )(packed, *prev)


def pack_body(wg_ref, wu_ref, wd_ref, p_ref):
    for c in range(12):
        p_ref[0, c * 72:c * 72 + 36, :] = wg_ref[0, :, c * 128:(c + 1) * 128]
        p_ref[0, c * 72 + 36:c * 72 + 72, :] = wu_ref[0, :, c * 128:(c + 1) * 128]
    for b in range(4):
        p_ref[0, 864 + 96 * b:864 + 96 * b + 96, :] = wd_ref[0, :, b * 128:(b + 1) * 128]
    p_ref[0, 1248:1296, :] = jnp.concatenate([wd_ref[0, 0:48, 512:576], wd_ref[0, 48:96, 512:576]], axis=1)


def pack_weights(wg, wu, wd):
    return pl.pallas_call(
        pack_body,
        grid=(LAYERS,),
        in_specs=[
            rows_spec(1, 36, FFN),
            rows_spec(1, 36, FFN),
            rows_spec(1, 96, DIM),
        ],
        out_specs=rows_spec(1, PROWS, 128),
        out_shape=jax.ShapeDtypeStruct((LAYERS, PROWS, 128), BF),
        name='pack_weights',
    )(wg, wu, wd)


def unpack_weights(p_ref, slot, wg_s, wu_s, wd_s):
    for d in range(N_DEV):
        for c in range(12):
            cols = slice(c * 128, (c + 1) * 128)
            wg_s[36 * d:36 * d + 36, cols] = p_ref[d, slot, c * 72:c * 72 + 36, :]
            wu_s[36 * d:36 * d + 36, cols] = p_ref[d, slot, c * 72 + 36:c * 72 + 72, :]
        for b in range(4):
            wd_s[96 * d:96 * d + 96, 128 * b:128 * b + 128] = p_ref[d, slot, 864 + 96 * b:864 + 96 * b + 96, :]
        tail = p_ref[d, slot, 1248:1296, :]
        wd_s[96 * d:96 * d + 48, 512:576] = tail[:, :64]
        wd_s[96 * d + 48:96 * d + 96, 512:576] = tail[:, 64:]


GROUPS = ((4, 3), (2, 1, 0))


def solution(mesh):
    def device_step(hidden, w_gate, w_up, w_down, w_out, targets, loss_mask):
        me = lax.axis_index(AXIS)
        gather = functools.partial(lax.all_gather, axis_name=AXIS)
        barrier = lax.optimization_barrier
        lab = jnp.concatenate([targets.astype(F32)[None], loss_mask.astype(F32)[None], jnp.zeros((6, TOK), F32)], axis=0)
        lab = gather_labels(lab)
        packs = pack_weights(w_gate, w_up, w_down)
        pack_top = gather(packs[4:])
        w_vocab = lax.all_to_all(w_out.reshape(36, N_DEV, VLOC), AXIS, 1, 0).reshape(DIM, VLOC)
        pack_top, w_vocab, lab = barrier((pack_top, w_vocab, lab))
        t, z_packed = top_forward(hidden[4], pack_top)

        mask = lab[:, 1, :]
        w_tok = mask / jnp.sum(mask)
        tgt = lab[:, 0, :] - (me * VLOC).astype(F32)
        w_own = lax.dynamic_slice(w_tok, (me, 0), (1, TOK))

        z_all = [gather(z_packed[c]) for c in range(CHUNKS)]
        rest = gather(packs[:4])
        acc, loss, dz_own = None, jnp.zeros((), F32), []
        for c in range(CHUNKS):
            sl = slice(c * TB, (c + 1) * TB)
            zero = jnp.zeros((6, CHUNK_TOK), F32)
            tok = jnp.concatenate([tgt[:, sl].reshape(1, CHUNK_TOK), w_tok[:, sl].reshape(1, CHUNK_TOK), zero], axis=0)
            if c == 1:
                tok, acc, rest = barrier((tok, acc, rest))
            e, ms, st = head_pass1(z_all[c], w_vocab, tok)
            res = exchange_stats(st, w_own[:, sl], 2 + c)
            loss = loss + jnp.sum(res[2])
            dz, acc = head_pass2(z_all[c], w_vocab, tok, res, e, ms, acc)
            if c == 1:
                dz, dz_own[0] = barrier((dz, dz_own[0]))
            dz_own.append(lax.psum_scatter(dz, AXIS, scatter_dimension=0, tiled=False))
        acc, dz_own[1] = barrier((acc, dz_own[1]))
        grad_out = lax.all_to_all(acc.reshape(N_DEV, 36, VLOC), AXIS, 0, 1)

        g_args = [t, *dz_own]
        outs, red = None, None
        for group in GROUPS:
            buf = None
            for i, l in enumerate(group):
                pk, ws = (pack_top, 0) if l == 4 else (rest, l)
                g, buf = block_backward(hidden[l], pk, ws, g_args, buf, i, len(group), BF if l == 0 else F32)
                g_args = [g]
            if red is not None:
                buf, red, grad_out = barrier((buf, red, grad_out))
                outs = unpack_grads(red, GROUPS[0], None)
            red = lax.psum_scatter(buf, AXIS, scatter_dimension=0, tiled=False)
        grad_gate, grad_up, grad_down = unpack_grads(red, GROUPS[1], outs)
        grad_out = grad_out.reshape(36, VOCAB)
        return grad_gate, grad_up, grad_down, grad_out, g, loss

    stacked = P(None, AXIS, None)
    row = P(AXIS, None)
    return jax.shard_map(device_step, mesh=mesh, in_specs=(stacked, stacked, stacked, stacked, row, P(AXIS), P(AXIS)), out_specs=(stacked, stacked, stacked, row, row, P()), check_vma=False)
```

```python
import functools

import jax
import jax.numpy as jnp
from jax import lax
from jax.experimental import pallas as pl
from jax.experimental.pallas import tpu as pltpu
from jax.sharding import PartitionSpec as P

EPS = 1e-5
AXIS = 'fsdp'
N_DEV = 16
LAYERS = 5
TOK = 1024
DIM = 576
FFN = 1536
VOCAB = 49152
VLOC = VOCAB // N_DEV
TOKENS = TOK * N_DEV
SPLITS = ((0, 640), (640, 384))
STRIPS = 4
SW = VLOC // STRIPS
PROWS = 1296
BF = jnp.bfloat16
F32 = jnp.float32
MESH = pl.DeviceIdType.MESH
LANE = 128
D4 = 4 * LANE
HL = LANE // 2
Q = DIM // N_DEV
Q2 = 2 * Q
PD = FFN // N_DEV
PH = PD // 2
A0 = 12 * Q2
TL0 = A0 + 4 * PD
VMEM_LIMIT = 62 * 1024 * 1024


def whole(*shape):
    return pl.BlockSpec(shape, lambda i: tuple(0 * d for d in shape))


def rows_spec(*shape):
    rest = shape[1:]
    return pl.BlockSpec(shape, lambda i: (i, *(0 * d for d in rest)))


def lanes_spec(*shape):
    return pl.BlockSpec(shape, lambda i: (0, i))


VM = pl.BlockSpec(memory_space=pltpu.VMEM)
HB = pl.BlockSpec(memory_space=pl.ANY)


def dot_nn(a, b):
    return lax.dot_general(a, b, (((1,), (0,)), ((), ())), preferred_element_type=F32)


def dot_nt(a, b):
    return lax.dot_general(a, b, (((1,), (1,)), ((), ())), preferred_element_type=F32)


def dot_tn(a, b):
    return lax.dot_general(a, b, (((0,), (0,)), ((), ())), preferred_element_type=F32)


def inv_rms_of(x):
    return lax.rsqrt(jnp.mean(x * x, axis=-1, keepdims=True) + EPS)


def norm_grad(x, e):
    r = inv_rms_of(x)
    return r * e - x * (r * r * r) * jnp.mean(x * e, axis=-1, keepdims=True)


def store_packed(ref, val, rows):
    half = rows // 2
    for c in range(4):
        ref[0, c * rows:(c + 1) * rows, :] = val[:, c * LANE:(c + 1) * LANE]
    ref[0, 4 * rows:4 * rows + half, :] = jnp.concatenate([val[:half, D4:], val[half:, D4:]], axis=1)


def load_packed(dst, ref, rows):
    half = rows // 2
    for c in range(4):
        dst[:, c * LANE:(c + 1) * LANE] = ref[0, c * rows:(c + 1) * rows, :]
    tail = ref[0, 4 * rows:4 * rows + half, :]
    dst[0:half, D4:DIM] = tail[:, :HL]
    dst[half:rows, D4:DIM] = tail[:, HL:]


def unpack_rows(p, rows):
    half = rows // 2
    tail = p[4 * rows:]
    tail = jnp.concatenate([tail[:, :HL], tail[:, HL:]], axis=0)
    return jnp.concatenate([p[c * rows:(c + 1) * rows] for c in range(4)] + [tail], axis=1)


W_SCRATCH = [pltpu.VMEM((DIM, FFN), BF), pltpu.VMEM((DIM, FFN), BF), pltpu.VMEM((FFN, DIM), BF)]


def fwd_body(h_ref, p_ref, t_ref, z0_ref, z1_ref, wg_ref, wu_ref, wd_ref):
    unpack_weights(p_ref, 0, wg_ref, wu_ref, wd_ref)
    for (off, tb), z_ref in zip(SPLITS, (z0_ref, z1_ref)):
        rows = slice(off, off + tb)
        h = h_ref[rows, :].astype(F32)
        n = (h * inv_rms_of(h)).astype(BF)
        u = dot_nn(n, wg_ref[...])
        v = dot_nn(n, wu_ref[...])
        a = (u * jax.nn.sigmoid(u) * v).astype(BF)
        t = (h + dot_nn(a, wd_ref[...])).astype(BF)
        t_ref[rows, :] = t
        t = t.astype(F32)
        store_packed(z_ref, (t * inv_rms_of(t)).astype(BF), tb)


def packed_rows(tb):
    return tb * 9 // 2


def top_forward(h, packs):
    zs = [(1, packed_rows(tb), LANE) for _, tb in SPLITS]
    return pl.pallas_call(
        fwd_body,
        grid=(1,),
        in_specs=[whole(TOK, DIM), whole(N_DEV, 1, PROWS, LANE)],
        out_specs=[whole(TOK, DIM)] + [whole(*z) for z in zs],
        out_shape=[jax.ShapeDtypeStruct((TOK, DIM), BF)] + [jax.ShapeDtypeStruct(z, BF) for z in zs],
        scratch_shapes=W_SCRATCH,
        compiler_params=pltpu.CompilerParams(vmem_limit_bytes=VMEM_LIMIT),
        cost_estimate=pl.CostEstimate(flops=6 * TOK * DIM * FFN, bytes_accessed=10 * 2**20, transcendentals=TOK * FFN),
        name='top_forward',
    )(h, packs)


def peers_barrier(me):
    sem = pltpu.get_barrier_semaphore()
    for off in range(1, N_DEV):
        pl.semaphore_signal(sem, inc=1, device_id=(lax.rem(me + off, N_DEV),), device_id_type=MESH)
    pl.semaphore_wait(sem, N_DEV - 1)


def all_send(me, src_of, dst, send_sem, recv_sem):
    copies = []
    for off in range(1, N_DEV):
        to = lax.rem(me + off, N_DEV)
        copy = pltpu.make_async_remote_copy(
            src_ref=src_of(to), dst_ref=dst.at[me], send_sem=send_sem.at[off], recv_sem=recv_sem.at[me],
            device_id=(to,), device_id_type=MESH)
        copy.start()
        copies.append(copy)
    return copies


def all_wait(me, src_of, dst, send_sem, recv_sem):
    for off in range(1, N_DEV):
        frm = lax.rem(me + N_DEV - off, N_DEV)
        copy = pltpu.make_async_remote_copy(
            src_ref=src_of(frm), dst_ref=dst.at[frm], send_sem=send_sem.at[off], recv_sem=recv_sem.at[frm],
            device_id=(frm,), device_id_type=MESH)
        copy.wait_recv()


def labels_body(x_ref, o_ref, buf, send_sem, recv_sem):
    me = lax.axis_index(AXIS)
    peers_barrier(me)
    src = lambda j: x_ref
    copies = all_send(me, src, buf, send_sem, recv_sem)
    all_wait(me, src, buf, send_sem, recv_sem)
    for copy in copies:
        copy.wait_send()
    for j in range(N_DEV):
        o_ref[j] = jnp.where(me == j, x_ref[...], buf[j])


def gather_labels(x):
    return pl.pallas_call(
        labels_body,
        in_specs=[VM],
        out_specs=VM,
        out_shape=jax.ShapeDtypeStruct((N_DEV, 8, TOK), F32),
        scratch_shapes=[pltpu.VMEM((N_DEV, 8, TOK), F32), pltpu.SemaphoreType.DMA((N_DEV,)), pltpu.SemaphoreType.DMA((N_DEV,))],
        compiler_params=pltpu.CompilerParams(collective_id=1, has_side_effects=True),
        cost_estimate=pl.CostEstimate(flops=2 * 10**9, bytes_accessed=2**20, transcendentals=0),
        name='gather_labels',
    )(x)


def stats_body(st_ref, w_ref, o_ref, buf1, own, buf2, send1, recv1, send2, recv2):
    me = lax.axis_index(AXIS)
    TB = w_ref.shape[1]
    peers_barrier(me)
    part = lambda j: st_ref.at[:, pl.ds(pl.multiple_of(j * TB, TB), TB)]
    copies = all_send(me, part, buf1, send1, recv1)
    all_wait(me, part, buf1, send1, recv1)
    mine = st_ref[:, pl.ds(pl.multiple_of(me * TB, TB), TB)]
    rows = [jnp.where(me == j, mine, buf1[j]) for j in range(N_DEV)]
    m = functools.reduce(jnp.maximum, [r[0:1] for r in rows])
    s = sum(r[1:2] * jnp.exp(r[0:1] - m) for r in rows)
    t = sum(r[2:3] for r in rows)
    own[...] = jnp.concatenate([m, 1.0 / s, w_ref[0:1, :] * (m + jnp.log(s) - t), jnp.zeros((5, TB), F32)], axis=0)
    src = lambda j: own
    copies += all_send(me, src, buf2, send2, recv2)
    all_wait(me, src, buf2, send2, recv2)
    for copy in copies:
        copy.wait_send()
    for j in range(N_DEV):
        o_ref[:, j * TB:(j + 1) * TB] = jnp.where(me == j, own[...], buf2[j])


def exchange_stats(st, w_own, cid):
    TB = w_own.shape[1]
    return pl.pallas_call(
        stats_body,
        in_specs=[VM, VM],
        out_specs=VM,
        out_shape=jax.ShapeDtypeStruct(st.shape, F32),
        scratch_shapes=[
            pltpu.VMEM((N_DEV, 8, TB), F32), pltpu.VMEM((8, TB), F32), pltpu.VMEM((N_DEV, 8, TB), F32),
            pltpu.SemaphoreType.DMA((N_DEV,)), pltpu.SemaphoreType.DMA((N_DEV,)),
            pltpu.SemaphoreType.DMA((N_DEV,)), pltpu.SemaphoreType.DMA((N_DEV,)),
        ],
        compiler_params=pltpu.CompilerParams(collective_id=cid, has_side_effects=True),
        cost_estimate=pl.CostEstimate(flops=2 * 10**9, bytes_accessed=2**20, transcendentals=0),
        name='exchange_stats',
    )(st, w_own)


def pass1_body(z_ref, w_ref, tok_ref, e_ref, ms_ref, st_ref, z_s):
    TB = z_s.shape[0]
    load_packed(z_s, z_ref, TB)
    z = z_s[...]
    tokc = jnp.concatenate([tok_ref[...], jnp.zeros((120, TB), F32)], axis=0).T
    tgt = tokc[:, 0:1]
    lane = lax.broadcasted_iota(jnp.int32, (TB, LANE), 1)
    ids = lax.broadcasted_iota(jnp.int32, (1, SW), 1).astype(F32)
    ms = jnp.zeros((TB, LANE), F32)
    tl = jnp.zeros((TB, 1), F32)
    m_list, s_list = [], []
    for s in range(STRIPS):
        l = dot_nn(z, w_ref[:, s * SW:(s + 1) * SW])
        m = jnp.max(l, axis=1, keepdims=True)
        e = jnp.exp(l - m)
        e_ref[:, s * SW:(s + 1) * SW] = e
        s_list.append(jnp.sum(e, axis=1, keepdims=True))
        m_list.append(m)
        tl = tl + jnp.sum(jnp.where(ids == tgt - float(s * SW), l, 0.0), axis=1, keepdims=True)
        ms = jnp.where(lane == s, m, ms)
    m_all = functools.reduce(jnp.maximum, m_list)
    s_all = sum(sv * jnp.exp(mv - m_all) for sv, mv in zip(s_list, m_list))
    ms_ref[...] = ms
    st = jnp.where(lane == 0, m_all, jnp.where(lane == 1, s_all, jnp.where(lane == 2, tl, 0.0)))
    st_ref[...] = st.T[0:8, :]


def head_pass1(z_all, w, tok):
    CHUNK_TOK = tok.shape[1]
    TB = CHUNK_TOK // N_DEV
    ZROWS = packed_rows(TB)
    return pl.pallas_call(
        pass1_body,
        grid=(N_DEV,),
        in_specs=[
            rows_spec(1, ZROWS, LANE),
            whole(DIM, VLOC),
            lanes_spec(8, TB),
        ],
        out_specs=[
            rows_spec(TB, VLOC),
            rows_spec(TB, LANE),
            lanes_spec(8, TB),
        ],
        out_shape=[
            jax.ShapeDtypeStruct((CHUNK_TOK, VLOC), F32),
            jax.ShapeDtypeStruct((CHUNK_TOK, LANE), F32),
            jax.ShapeDtypeStruct((8, CHUNK_TOK), F32),
        ],
        scratch_shapes=[pltpu.VMEM((TB, DIM), BF)],
        compiler_params=pltpu.CompilerParams(vmem_limit_bytes=VMEM_LIMIT),
        cost_estimate=pl.CostEstimate(flops=2 * CHUNK_TOK * DIM * VLOC, bytes_accessed=4 * CHUNK_TOK * VLOC, transcendentals=CHUNK_TOK * VLOC),
        name='head_pass1',
    )(z_all, w, tok)


def pass2_body(has_acc, *refs):
    if has_acc:
        z_ref, w_ref, tok_ref, res_ref, e_ref, ms_ref, acc_ref, dz_ref, gw_ref, z_s, q_s = refs
    else:
        z_ref, w_ref, tok_ref, res_ref, e_ref, ms_ref, dz_ref, gw_ref, z_s, q_s = refs
        acc_ref = None

    @pl.when(pl.program_id(0) == 0)
    def _():
        if has_acc:
            gw_ref[...] = acc_ref[...]
        else:
            gw_ref[...] = jnp.zeros_like(gw_ref)

    TB = z_s.shape[0]
    load_packed(z_s, z_ref, TB)
    z = z_s[...]
    tokc = jnp.concatenate([tok_ref[...], res_ref[...], jnp.zeros((112, TB), F32)], axis=0).T
    tgt, w_tok, m_glob, s_inv = (tokc[:, i:i + 1] for i in (0, 1, 8, 9))
    ids = lax.broadcasted_iota(jnp.int32, (1, SW), 1).astype(F32)
    for s in range(STRIPS):
        cols = slice(s * SW, (s + 1) * SW)
        scale = jnp.exp(ms_ref[:, s:s + 1] - m_glob) * s_inv
        p = e_ref[:, cols] * scale
        p = jnp.where(ids == tgt - float(s * SW), p - 1.0, p)
        q = (w_tok * p).astype(BF)
        q_s[:, cols] = q
        gw_ref[:, cols] += dot_tn(z, q)
    dz = dot_nt(q_s[...], w_ref[...])
    store_packed(dz_ref, dz, TB)


def head_pass2(z_all, w, tok, res, e, ms, acc):
    CHUNK_TOK = tok.shape[1]
    TB = CHUNK_TOK // N_DEV
    ZROWS = packed_rows(TB)
    in_specs = [
        rows_spec(1, ZROWS, LANE),
        whole(DIM, VLOC),
        lanes_spec(8, TB),
        lanes_spec(8, TB),
        rows_spec(TB, VLOC),
        rows_spec(TB, LANE),
    ]
    args = [z_all, w, tok, res, e, ms]
    if acc is not None:
        in_specs.append(pl.BlockSpec((DIM, VLOC), lambda i: (0, 0), pipeline_mode=pl.Buffered(1)))
        args.append(acc)
    return pl.pallas_call(
        functools.partial(pass2_body, acc is not None),
        grid=(N_DEV,),
        in_specs=in_specs,
        out_specs=[
            rows_spec(1, ZROWS, LANE),
            pl.BlockSpec((DIM, VLOC), lambda i: (0, 0), pipeline_mode=pl.Buffered(1)),
        ],
        out_shape=[
            jax.ShapeDtypeStruct((N_DEV, ZROWS, LANE), F32),
            jax.ShapeDtypeStruct((DIM, VLOC), F32),
        ],
        scratch_shapes=[pltpu.VMEM((TB, DIM), BF), pltpu.VMEM((TB, VLOC), BF)],
        compiler_params=pltpu.CompilerParams(vmem_limit_bytes=VMEM_LIMIT),
        cost_estimate=pl.CostEstimate(flops=4 * CHUNK_TOK * DIM * VLOC, bytes_accessed=4 * CHUNK_TOK * VLOC, transcendentals=0),
        name='head_pass2',
    )(*args)


def bwd_body(top, off, *refs):
    if top:
        h_ref, p_ref, t_ref, d0_ref, d1_ref, go_ref, buf_ref, *scratch = refs
    else:
        h_ref, p_ref, g_ref, buf_in, go_ref, buf_ref, *scratch = refs
    _, wg_ref, wu_ref, wd_ref, n_s, k_s, a_s, du_s, dv_s, pk_s, sem = scratch
    unpack_weights(p_ref, 0, wg_ref, wu_ref, wd_ref)

    for i, (lo, tb) in enumerate(SPLITS):
        rows = slice(lo, lo + tb)
        h = h_ref[rows, :].astype(F32)
        r = inv_rms_of(h)
        n = (h * r).astype(BF)
        if top:
            g = norm_grad(t_ref[rows, :].astype(F32), unpack_rows((d0_ref, d1_ref)[i], tb))
        else:
            g = g_ref[rows, :]
        k = g.astype(BF)
        u = dot_nn(n, wg_ref[...])
        v = dot_nn(n, wu_ref[...])
        e = dot_nt(k, wd_ref[...])
        sg = jax.nn.sigmoid(u)
        us = u * sg
        a_s[rows, :] = (us * v).astype(BF)
        du = (e * v * sg * (1.0 + u * (1.0 - sg))).astype(BF)
        dv = (e * us).astype(BF)
        n_s[rows, :] = n
        k_s[rows, :] = k
        du_s[rows, :] = du
        dv_s[rows, :] = dv
        dn = dot_nt(du, wg_ref[...]) + dot_nt(dv, wu_ref[...])
        go_ref[rows, :] = (g + r * dn - h * (r * r * r) * jnp.mean(h * dn, axis=-1, keepdims=True)).astype(go_ref.dtype)

    n = n_s[...]
    k = k_s[...]
    for c in range(6):
        gg = dot_tn(n, du_s[:, c * 256:(c + 1) * 256])
        gu = dot_tn(n, dv_s[:, c * 256:(c + 1) * 256])
        for j in range(2):
            base = (2 * c + j) * Q2
            for d in range(N_DEV):
                pk_s[d, base:base + Q, :] = gg[Q * d:Q * d + Q, j * LANE:(j + 1) * LANE]
                pk_s[d, base + Q:base + Q2, :] = gu[Q * d:Q * d + Q, j * LANE:(j + 1) * LANE]
    copy_a = pltpu.make_async_copy(pk_s.at[:, pl.ds(0, A0), :], buf_ref.at[:, pl.ds(off, A0), :], sem.at[0])
    copy_a.start()
    for c in range(4):
        gd = dot_tn(a_s[:, c * 384:(c + 1) * 384], k)
        for j in range(4):
            d = c * 4 + j
            x = gd[PD * j:PD * j + PD, :]
            for b in range(4):
                pk_s[d, A0 + PD * b:A0 + PD * b + PD, :] = x[:, LANE * b:LANE * b + LANE]
            pk_s[d, TL0:1296, :] = jnp.concatenate([x[:PH, D4:], x[PH:, D4:]], axis=1)
    copy_b = pltpu.make_async_copy(pk_s.at[:, pl.ds(A0, 432), :], buf_ref.at[:, pl.ds(off + A0, 432), :], sem.at[1])
    copy_b.start()
    copy_a.wait()
    copy_b.wait()


def block_backward(h, packs, wslot, g_args, buf, slot, slots, out_dtype):
    top = len(g_args) == 3
    args = [h, packs, *g_args]
    in_specs = [whole(TOK, DIM), pl.BlockSpec((N_DEV, 1, PROWS, LANE), lambda i: (0, wslot, 0, 0))]
    in_specs += [whole(*x.shape) for x in g_args]
    aliases = {}
    if not top:
        args.append(jnp.zeros((8, LANE), F32) if buf is None else buf)
        in_specs.append(HB)
        aliases = {} if buf is None else {3: 1}
    return pl.pallas_call(
        functools.partial(bwd_body, top, slot * PROWS),
        grid=(1,),
        in_specs=in_specs,
        out_specs=[whole(TOK, DIM), HB],
        out_shape=[jax.ShapeDtypeStruct((TOK, DIM), out_dtype), jax.ShapeDtypeStruct((N_DEV, slots * PROWS, LANE), F32)],
        scratch_shapes=[pltpu.SMEM((1,), jnp.int32)] + W_SCRATCH + [
            pltpu.VMEM((TOK, DIM), BF), pltpu.VMEM((TOK, DIM), BF), pltpu.VMEM((TOK, FFN), BF),
            pltpu.VMEM((TOK, FFN), BF), pltpu.VMEM((TOK, FFN), BF), pltpu.VMEM((N_DEV, PROWS, LANE), F32),
            pltpu.SemaphoreType.DMA((2,)),
        ],
        input_output_aliases=aliases,
        compiler_params=pltpu.CompilerParams(vmem_limit_bytes=VMEM_LIMIT),
        cost_estimate=pl.CostEstimate(flops=16 * TOK * DIM * FFN, bytes_accessed=24 * 2**20, transcendentals=TOK * FFN),
        name='block_backward',
    )(*args)


def cube_body(pieces, x_ref, o_ref, own, r0, r1, r2, r3, send, recv, local):
    me = lax.axis_index(AXIS)
    pos = [me // 8, me // 4 % 2, me // 2 % 2, me % 2]
    weight = (8, 4, 2, 1)
    mate = [me + w * (1 - 2 * p) for w, p in zip(weight, pos)]
    sem = pltpu.get_barrier_semaphore()
    for j in mate:
        pl.semaphore_signal(sem, inc=1, device_id=(j,), device_id_type=MESH)
    pl.semaphore_wait(sem, 4)
    core = pos[3]
    size = o_ref.shape[0] // (3 * pieces)
    units = [(k, (k + 3 * p) * size) for p in range(pieces) for k in range(3)]

    def pick(ref, k, stage, rows, flip):
        index = [slice(None)] * 3
        for j in range(stage):
            d = (k + j) % 3
            index[d] = pos[d]
        d = (k + stage) % 3
        index[d] = 1 - pos[d] if flip else pos[d]
        return ref.at[(*index, rows)]

    def landing(k, stage, rows):
        return (r1.at[:, :, rows], r2.at[:, rows], r3.at[rows])[stage]

    def first(u):
        k, base = units[u]
        rows = pl.ds(base, size)
        out = pltpu.make_async_remote_copy(
            src_ref=x_ref.at[:, :, :, 1 - core, rows], dst_ref=r0.at[:, :, :, rows], send_sem=send.at[0, u],
            recv_sem=recv.at[0, u], device_id=(mate[3],), device_id_type=MESH)
        return out, pltpu.make_async_copy(x_ref.at[:, :, :, core, rows], own.at[:, :, :, rows], local.at[u])

    def later(u, stage):
        k, base = units[u]
        rows = pl.ds(base, size)
        return pltpu.make_async_remote_copy(
            src_ref=pick(own, k, stage, rows, True), dst_ref=landing(k, stage, rows), send_sem=send.at[stage + 1, u],
            recv_sem=recv.at[stage + 1, u], device_id=(mate[(k + stage) % 3],), device_id_type=MESH)

    def add(dst, src):
        step = PH

        def body(i, carry):
            rows = pl.ds(pl.multiple_of(i * step, step), step)
            lead = (slice(None),) * (len(dst.shape) - 2)
            dst[(*lead, rows)] += src[(*lead, rows)]
            return carry

        lax.fori_loop(0, size // step, body, 0)

    many = range(len(units))
    for u in many:
        for copy in first(u):
            copy.start()
    for stage in range(4):
        for u in many:
            k, base = units[u]
            rows = pl.ds(base, size)
            if stage == 0:
                out, loc = first(u)
                loc.wait()
                out.wait_recv()
                add(own.at[:, :, :, rows], r0.at[:, :, :, rows])
            else:
                later(u, stage - 1).wait_recv()
                add(pick(own, k, stage - 1, rows, False), landing(k, stage - 1, rows))
            if stage < 3:
                if u > 0:
                    later(u - 1, stage).start()
                if u == many[-1]:
                    later(u, stage).start()
            else:
                o_ref[rows, :] = own[(*pos[:3], rows)]
    for u in many:
        first(u)[0].wait_send()
        for stage in range(3):
            later(u, stage).wait_send()


def cube_reduce_scatter(x, pieces, cid):
    rows = x.shape[1]
    units = 3 * pieces
    return pl.pallas_call(
        functools.partial(cube_body, pieces),
        in_specs=[HB],
        out_specs=VM,
        out_shape=jax.ShapeDtypeStruct((rows, LANE), F32),
        scratch_shapes=[
            pltpu.VMEM((2, 2, 2, rows, LANE), F32), pltpu.VMEM((2, 2, 2, rows, LANE), F32), pltpu.VMEM((2, 2, rows, LANE), F32),
            pltpu.VMEM((2, rows, LANE), F32), pltpu.VMEM((rows, LANE), F32),
            pltpu.SemaphoreType.DMA((4, units)), pltpu.SemaphoreType.DMA((4, units)), pltpu.SemaphoreType.DMA((units,)),
        ],
        compiler_params=pltpu.CompilerParams(collective_id=cid, has_side_effects=True, vmem_limit_bytes=VMEM_LIMIT),
        cost_estimate=pl.CostEstimate(flops=50 * 10**9, bytes_accessed=2**20, transcendentals=0),
        name='cube_reduce_scatter',
    )(x.reshape(2, 2, 2, 2, rows, LANE))


def unpack_body(has_prev, p_ref, *refs):
    gg_ref, gu_ref, gd_ref = refs[3:] if has_prev else refs
    for c in range(12):
        gg_ref[0, :, c * LANE:(c + 1) * LANE] = p_ref[c * Q2:c * Q2 + Q, :]
        gu_ref[0, :, c * LANE:(c + 1) * LANE] = p_ref[c * Q2 + Q:c * Q2 + Q2, :]
    for b in range(4):
        gd_ref[0, :, b * LANE:(b + 1) * LANE] = p_ref[A0 + PD * b:A0 + PD * b + PD, :]
    tail = p_ref[TL0:1296, :]
    gd_ref[0, 0:PH, D4:DIM] = tail[:, :HL]
    gd_ref[0, PH:PD, D4:DIM] = tail[:, HL:]


def unpack_grads(packed, group, prev):
    prev = list(prev or ())
    back = lambda i: (group[0] - i, 0, 0)
    return pl.pallas_call(
        functools.partial(unpack_body, bool(prev)),
        grid=(len(group),),
        in_specs=[rows_spec(PROWS, LANE)] + [HB] * len(prev),
        out_specs=[
            pl.BlockSpec((1, Q, FFN), back),
            pl.BlockSpec((1, Q, FFN), back),
            pl.BlockSpec((1, PD, DIM), back),
        ],
        out_shape=[
            jax.ShapeDtypeStruct((LAYERS, Q, FFN), F32),
            jax.ShapeDtypeStruct((LAYERS, Q, FFN), F32),
            jax.ShapeDtypeStruct((LAYERS, PD, DIM), F32),
        ],
        input_output_aliases={1 + i: i for i in range(len(prev))},
        name='unpack_grads',
    )(packed, *prev)


def pack_body(wg_ref, wu_ref, wd_ref, p_ref):
    for c in range(12):
        p_ref[0, c * Q2:c * Q2 + Q, :] = wg_ref[0, :, c * LANE:(c + 1) * LANE]
        p_ref[0, c * Q2 + Q:c * Q2 + Q2, :] = wu_ref[0, :, c * LANE:(c + 1) * LANE]
    for b in range(4):
        p_ref[0, A0 + PD * b:A0 + PD * b + PD, :] = wd_ref[0, :, b * LANE:(b + 1) * LANE]
    p_ref[0, TL0:1296, :] = jnp.concatenate([wd_ref[0, 0:PH, D4:DIM], wd_ref[0, PH:PD, D4:DIM]], axis=1)


def pack_weights(wg, wu, wd):
    return pl.pallas_call(
        pack_body,
        grid=(LAYERS,),
        in_specs=[
            rows_spec(1, Q, FFN),
            rows_spec(1, Q, FFN),
            rows_spec(1, PD, DIM),
        ],
        out_specs=rows_spec(1, PROWS, LANE),
        out_shape=jax.ShapeDtypeStruct((LAYERS, PROWS, LANE), BF),
        name='pack_weights',
    )(wg, wu, wd)


def unpack_weights(p_ref, slot, wg_s, wu_s, wd_s):
    for d in range(N_DEV):
        for c in range(12):
            cols = slice(c * LANE, (c + 1) * LANE)
            wg_s[Q * d:Q * d + Q, cols] = p_ref[d, slot, c * Q2:c * Q2 + Q, :]
            wu_s[Q * d:Q * d + Q, cols] = p_ref[d, slot, c * Q2 + Q:c * Q2 + Q2, :]
        for b in range(4):
            wd_s[PD * d:PD * d + PD, LANE * b:LANE * b + LANE] = p_ref[d, slot, A0 + PD * b:A0 + PD * b + PD, :]
        tail = p_ref[d, slot, TL0:1296, :]
        wd_s[PD * d:PD * d + PH, D4:DIM] = tail[:, :HL]
        wd_s[PD * d + PH:PD * d + PD, D4:DIM] = tail[:, HL:]


GROUPS = ((4, 3), (2, 1, 0))


def solution(mesh):
    def device_step(hidden, w_gate, w_up, w_down, w_out, targets, loss_mask):
        me = lax.axis_index(AXIS)
        gather = functools.partial(lax.all_gather, axis_name=AXIS)
        barrier = lax.optimization_barrier
        lab = jnp.concatenate([targets.astype(F32)[None], loss_mask.astype(F32)[None], jnp.zeros((6, TOK), F32)], axis=0)
        lab = gather_labels(lab)
        w_gate, lab = barrier((w_gate, lab))
        packs = pack_weights(w_gate, w_up, w_down)
        pack_top = gather(packs[4:])
        w_out, lab = barrier((w_out, lab))
        w_vocab = lax.all_to_all(w_out.reshape(Q, N_DEV, VLOC), AXIS, 1, 0).reshape(DIM, VLOC)
        pack_top, w_vocab, lab = barrier((pack_top, w_vocab, lab))
        t, *z_packed = top_forward(hidden[4], pack_top)

        mask = lab[:, 1, :]
        w_tok = mask / jnp.sum(mask)
        tgt = lab[:, 0, :] - (me * VLOC).astype(F32)
        w_own = lax.dynamic_slice(w_tok, (me, 0), (1, TOK))

        z_all = [lax.all_gather(z, AXIS, tiled=True) for z in z_packed]
        rest = gather(packs[:4])
        acc, loss, dz_own = None, jnp.zeros((), F32), []
        for c, (lo, tb) in enumerate(SPLITS):
            sl = slice(lo, lo + tb)
            CHUNK_TOK = tb * N_DEV
            zero = jnp.zeros((6, CHUNK_TOK), F32)
            tok = jnp.concatenate([tgt[:, sl].reshape(1, CHUNK_TOK), w_tok[:, sl].reshape(1, CHUNK_TOK), zero], axis=0)
            if c == 1:
                tok, acc, rest = barrier((tok, acc, rest))
            e, ms, st = head_pass1(z_all[c], w_vocab, tok)
            res = exchange_stats(st, w_own[:, sl], 2 + c)
            loss = loss + jnp.sum(res[2])
            dz, acc = head_pass2(z_all[c], w_vocab, tok, res, e, ms, acc)
            if c == 1:
                dz, dz_own[0] = barrier((dz, dz_own[0]))
                dz_own.append(cube_reduce_scatter(dz, 2, 4))
            else:
                dz_own.append(lax.psum_scatter(dz, AXIS, scatter_dimension=0, tiled=False))
        acc, dz_own[1] = barrier((acc, dz_own[1]))
        grad_out = lax.all_to_all(acc.reshape(N_DEV, Q, VLOC), AXIS, 0, 1)

        g_args = [t, *dz_own]
        bufs = []
        for group in GROUPS:
            buf = None
            for i, l in enumerate(group):
                pk, ws = (pack_top, 0) if l == 4 else (rest, l)
                g, buf = block_backward(hidden[l], pk, ws, g_args, buf, i, len(group), BF if l == 0 else F32)
                g_args = [g]
            bufs.append(buf)
        red = lax.psum_scatter(bufs[0], AXIS, scatter_dimension=0, tiled=False)
        red_low = cube_reduce_scatter(bufs[1], 3, 5)
        red, grad_out, red_low = barrier((red, grad_out, red_low))
        outs = unpack_grads(red, GROUPS[0], None)
        grad_gate, grad_up, grad_down = unpack_grads(red_low, GROUPS[1], outs)
        grad_out = grad_out.reshape(Q, VOCAB)
        return grad_gate, grad_up, grad_down, grad_out, g, loss

    stacked = P(None, AXIS, None)
    row = P(AXIS, None)
    return jax.shard_map(device_step, mesh=mesh, in_specs=(stacked, stacked, stacked, stacked, row, P(AXIS), P(AXIS)), out_specs=(stacked, stacked, stacked, row, row, P()), check_vma=False)
```

```python
import functools

import jax
import jax.numpy as jnp
from jax import lax
from jax.experimental import pallas as pl
from jax.experimental.pallas import tpu as pltpu
from jax.sharding import PartitionSpec as P

EPS = 1e-5
AXIS = 'fsdp'
N_DEV = 16
LAYERS = 5
TOK = 1024
DIM = 576
FFN = 1536
VOCAB = 49152
VLOC = VOCAB // N_DEV
TOKENS = TOK * N_DEV
SPLITS = ((0, 640), (640, 384))
STRIPS = 4
SW = VLOC // STRIPS
PROWS = 1296
BF = jnp.bfloat16
F32 = jnp.float32
MESH = pl.DeviceIdType.MESH
LANE = 128
D4 = 4 * LANE
HL = LANE // 2
Q = DIM // N_DEV
Q2 = 2 * Q
PD = FFN // N_DEV
PH = PD // 2
A0 = 12 * Q2
GROWS = VLOC // LANE * Q
TL0 = A0 + 4 * PD
VMEM_LIMIT = 62 * 1024 * 1024


def whole(*shape):
    return pl.BlockSpec(shape, lambda i: tuple(0 * d for d in shape))


def rows_spec(*shape):
    rest = shape[1:]
    return pl.BlockSpec(shape, lambda i: (i, *(0 * d for d in rest)))


def lanes_spec(*shape):
    return pl.BlockSpec(shape, lambda i: (0, i))


VM = pl.BlockSpec(memory_space=pltpu.VMEM)
HB = pl.BlockSpec(memory_space=pl.ANY)


def dot_nn(a, b):
    return lax.dot_general(a, b, (((1,), (0,)), ((), ())), preferred_element_type=F32)


def dot_nt(a, b):
    return lax.dot_general(a, b, (((1,), (1,)), ((), ())), preferred_element_type=F32)


def dot_tn(a, b):
    return lax.dot_general(a, b, (((0,), (0,)), ((), ())), preferred_element_type=F32)


def inv_rms_of(x):
    return lax.rsqrt(jnp.mean(x * x, axis=-1, keepdims=True) + EPS)


def norm_grad(x, e):
    r = inv_rms_of(x)
    return r * e - x * (r * r * r) * jnp.mean(x * e, axis=-1, keepdims=True)


def store_packed(ref, val, rows):
    half = rows // 2
    for c in range(4):
        ref[0, c * rows:(c + 1) * rows, :] = val[:, c * LANE:(c + 1) * LANE]
    ref[0, 4 * rows:4 * rows + half, :] = jnp.concatenate([val[:half, D4:], val[half:, D4:]], axis=1)


def load_packed(dst, ref, rows):
    half = rows // 2
    for c in range(4):
        dst[:, c * LANE:(c + 1) * LANE] = ref[0, c * rows:(c + 1) * rows, :]
    tail = ref[0, 4 * rows:4 * rows + half, :]
    dst[0:half, D4:DIM] = tail[:, :HL]
    dst[half:rows, D4:DIM] = tail[:, HL:]


def unpack_rows(p, rows):
    half = rows // 2
    tail = p[4 * rows:]
    tail = jnp.concatenate([tail[:, :HL], tail[:, HL:]], axis=0)
    return jnp.concatenate([p[c * rows:(c + 1) * rows] for c in range(4)] + [tail], axis=1)


W_SCRATCH = [pltpu.VMEM((DIM, FFN), BF), pltpu.VMEM((DIM, FFN), BF), pltpu.VMEM((FFN, DIM), BF)]


def fwd_body(h_ref, p_ref, t_ref, z0_ref, z1_ref, wg_ref, wu_ref, wd_ref):
    unpack_weights(p_ref, 0, wg_ref, wu_ref, wd_ref)
    for (off, tb), z_ref in zip(SPLITS, (z0_ref, z1_ref)):
        rows = slice(off, off + tb)
        h = h_ref[rows, :].astype(F32)
        n = (h * inv_rms_of(h)).astype(BF)
        u = dot_nn(n, wg_ref[...])
        v = dot_nn(n, wu_ref[...])
        a = (u * jax.nn.sigmoid(u) * v).astype(BF)
        t = (h + dot_nn(a, wd_ref[...])).astype(BF)
        t_ref[rows, :] = t
        t = t.astype(F32)
        store_packed(z_ref, (t * inv_rms_of(t)).astype(BF), tb)


def packed_rows(tb):
    return tb * 9 // 2


def top_forward(h, packs):
    zs = [(1, packed_rows(tb), LANE) for _, tb in SPLITS]
    return pl.pallas_call(
        fwd_body,
        grid=(1,),
        in_specs=[whole(TOK, DIM), whole(N_DEV, 1, PROWS, LANE)],
        out_specs=[whole(TOK, DIM)] + [whole(*z) for z in zs],
        out_shape=[jax.ShapeDtypeStruct((TOK, DIM), BF)] + [jax.ShapeDtypeStruct(z, BF) for z in zs],
        scratch_shapes=W_SCRATCH,
        compiler_params=pltpu.CompilerParams(vmem_limit_bytes=VMEM_LIMIT),
        cost_estimate=pl.CostEstimate(flops=6 * TOK * DIM * FFN, bytes_accessed=10 * 2**20, transcendentals=TOK * FFN),
        name='top_forward',
    )(h, packs)


def peers_barrier(me):
    sem = pltpu.get_barrier_semaphore()
    for off in range(1, N_DEV):
        pl.semaphore_signal(sem, inc=1, device_id=(lax.rem(me + off, N_DEV),), device_id_type=MESH)
    pl.semaphore_wait(sem, N_DEV - 1)


def all_send(me, src_of, dst, send_sem, recv_sem):
    copies = []
    for off in range(1, N_DEV):
        to = lax.rem(me + off, N_DEV)
        copy = pltpu.make_async_remote_copy(
            src_ref=src_of(to), dst_ref=dst.at[me], send_sem=send_sem.at[off], recv_sem=recv_sem.at[me],
            device_id=(to,), device_id_type=MESH)
        copy.start()
        copies.append(copy)
    return copies


def all_wait(me, src_of, dst, send_sem, recv_sem):
    for off in range(1, N_DEV):
        frm = lax.rem(me + N_DEV - off, N_DEV)
        copy = pltpu.make_async_remote_copy(
            src_ref=src_of(frm), dst_ref=dst.at[frm], send_sem=send_sem.at[off], recv_sem=recv_sem.at[frm],
            device_id=(frm,), device_id_type=MESH)
        copy.wait_recv()


def start_body(x_ref, w_ref, o_ref, wo_ref, buf, send_sem, recv_sem, send_w, recv_w, local):
    me = lax.axis_index(AXIS)
    peers_barrier(me)
    src = lambda j: x_ref
    part = lambda j: w_ref.at[:, pl.ds(pl.multiple_of(j * VLOC, VLOC), VLOC)]
    copies = all_send(me, src, buf, send_sem, recv_sem)
    copies += all_send(me, part, wo_ref, send_w, recv_w)
    mine = pltpu.make_async_copy(part(me), wo_ref.at[me], local)
    mine.start()
    all_wait(me, src, buf, send_sem, recv_sem)
    for j in range(N_DEV):
        o_ref[j] = jnp.where(me == j, x_ref[...], buf[j])
    all_wait(me, part, wo_ref, send_w, recv_w)
    mine.wait()
    for copy in copies:
        copy.wait_send()


def start_exchange(x, w):
    sems = pltpu.SemaphoreType.DMA((N_DEV,))
    return pl.pallas_call(
        start_body,
        in_specs=[VM, HB],
        out_specs=[VM, HB],
        out_shape=[jax.ShapeDtypeStruct((N_DEV, 8, TOK), F32), jax.ShapeDtypeStruct((N_DEV, Q, VLOC), BF)],
        scratch_shapes=[pltpu.VMEM((N_DEV, 8, TOK), F32), sems, sems, sems, sems, pltpu.SemaphoreType.DMA],
        compiler_params=pltpu.CompilerParams(collective_id=1, has_side_effects=True),
        cost_estimate=pl.CostEstimate(flops=50 * 10**9, bytes_accessed=2**20, transcendentals=0),
        name='start_exchange',
    )(x, w)


def stats_body(st_ref, w_ref, o_ref, buf1, own, buf2, send1, recv1, send2, recv2):
    me = lax.axis_index(AXIS)
    TB = w_ref.shape[1]
    peers_barrier(me)
    part = lambda j: st_ref.at[:, pl.ds(pl.multiple_of(j * TB, TB), TB)]
    copies = all_send(me, part, buf1, send1, recv1)
    all_wait(me, part, buf1, send1, recv1)
    mine = st_ref[:, pl.ds(pl.multiple_of(me * TB, TB), TB)]
    rows = [jnp.where(me == j, mine, buf1[j]) for j in range(N_DEV)]
    m = functools.reduce(jnp.maximum, [r[0:1] for r in rows])
    s = sum(r[1:2] * jnp.exp(r[0:1] - m) for r in rows)
    t = sum(r[2:3] for r in rows)
    own[...] = jnp.concatenate([m, 1.0 / s, w_ref[0:1, :] * (m + jnp.log(s) - t), jnp.zeros((5, TB), F32)], axis=0)
    src = lambda j: own
    copies += all_send(me, src, buf2, send2, recv2)
    all_wait(me, src, buf2, send2, recv2)
    for copy in copies:
        copy.wait_send()
    for j in range(N_DEV):
        o_ref[:, j * TB:(j + 1) * TB] = jnp.where(me == j, own[...], buf2[j])


def exchange_stats(st, w_own, cid):
    TB = w_own.shape[1]
    return pl.pallas_call(
        stats_body,
        in_specs=[VM, VM],
        out_specs=VM,
        out_shape=jax.ShapeDtypeStruct(st.shape, F32),
        scratch_shapes=[
            pltpu.VMEM((N_DEV, 8, TB), F32), pltpu.VMEM((8, TB), F32), pltpu.VMEM((N_DEV, 8, TB), F32),
            pltpu.SemaphoreType.DMA((N_DEV,)), pltpu.SemaphoreType.DMA((N_DEV,)),
            pltpu.SemaphoreType.DMA((N_DEV,)), pltpu.SemaphoreType.DMA((N_DEV,)),
        ],
        compiler_params=pltpu.CompilerParams(collective_id=cid, has_side_effects=True),
        cost_estimate=pl.CostEstimate(flops=2 * 10**9, bytes_accessed=2**20, transcendentals=0),
        name='exchange_stats',
    )(st, w_own)


def pass1_body(z_ref, w_ref, tok_ref, e_ref, ms_ref, st_ref, z_s):
    TB = z_s.shape[0]
    load_packed(z_s, z_ref, TB)
    z = z_s[...]
    tokc = jnp.concatenate([tok_ref[...], jnp.zeros((120, TB), F32)], axis=0).T
    tgt = tokc[:, 0:1]
    lane = lax.broadcasted_iota(jnp.int32, (TB, LANE), 1)
    ids = lax.broadcasted_iota(jnp.int32, (1, SW), 1).astype(F32)
    ms = jnp.zeros((TB, LANE), F32)
    tl = jnp.zeros((TB, 1), F32)
    m_list, s_list = [], []
    for s in range(STRIPS):
        l = dot_nn(z, w_ref[:, s * SW:(s + 1) * SW])
        m = jnp.max(l, axis=1, keepdims=True)
        e = jnp.exp(l - m)
        e_ref[:, s * SW:(s + 1) * SW] = e
        s_list.append(jnp.sum(e, axis=1, keepdims=True))
        m_list.append(m)
        tl = tl + jnp.sum(jnp.where(ids == tgt - float(s * SW), l, 0.0), axis=1, keepdims=True)
        ms = jnp.where(lane == s, m, ms)
    m_all = functools.reduce(jnp.maximum, m_list)
    s_all = sum(sv * jnp.exp(mv - m_all) for sv, mv in zip(s_list, m_list))
    ms_ref[...] = ms
    st = jnp.where(lane == 0, m_all, jnp.where(lane == 1, s_all, jnp.where(lane == 2, tl, 0.0)))
    st_ref[...] = st.T[0:8, :]


def head_pass1(z_all, w, tok):
    CHUNK_TOK = tok.shape[1]
    TB = CHUNK_TOK // N_DEV
    ZROWS = packed_rows(TB)
    return pl.pallas_call(
        pass1_body,
        grid=(N_DEV,),
        in_specs=[
            rows_spec(1, ZROWS, LANE),
            whole(DIM, VLOC),
            lanes_spec(8, TB),
        ],
        out_specs=[
            rows_spec(TB, VLOC),
            rows_spec(TB, LANE),
            lanes_spec(8, TB),
        ],
        out_shape=[
            jax.ShapeDtypeStruct((CHUNK_TOK, VLOC), F32),
            jax.ShapeDtypeStruct((CHUNK_TOK, LANE), F32),
            jax.ShapeDtypeStruct((8, CHUNK_TOK), F32),
        ],
        scratch_shapes=[pltpu.VMEM((TB, DIM), BF)],
        compiler_params=pltpu.CompilerParams(vmem_limit_bytes=VMEM_LIMIT),
        cost_estimate=pl.CostEstimate(flops=2 * CHUNK_TOK * DIM * VLOC, bytes_accessed=4 * CHUNK_TOK * VLOC, transcendentals=CHUNK_TOK * VLOC),
        name='head_pass1',
    )(z_all, w, tok)


def pass2_body(has_acc, *refs):
    if has_acc:
        z_ref, w_ref, tok_ref, res_ref, e_ref, ms_ref, acc_ref, dz_ref, pk_ref, z_s, q_s, gw_ref = refs
    else:
        z_ref, w_ref, tok_ref, res_ref, e_ref, ms_ref, dz_ref, gw_ref, z_s, q_s = refs
        acc_ref = None

    @pl.when(pl.program_id(0) == 0)
    def _():
        if has_acc:
            gw_ref[...] = acc_ref[...]
        else:
            gw_ref[...] = jnp.zeros_like(gw_ref)

    TB = z_s.shape[0]
    load_packed(z_s, z_ref, TB)
    z = z_s[...]
    tokc = jnp.concatenate([tok_ref[...], res_ref[...], jnp.zeros((112, TB), F32)], axis=0).T
    tgt, w_tok, m_glob, s_inv = (tokc[:, i:i + 1] for i in (0, 1, 8, 9))
    ids = lax.broadcasted_iota(jnp.int32, (1, SW), 1).astype(F32)
    for s in range(STRIPS):
        cols = slice(s * SW, (s + 1) * SW)
        scale = jnp.exp(ms_ref[:, s:s + 1] - m_glob) * s_inv
        p = e_ref[:, cols] * scale
        p = jnp.where(ids == tgt - float(s * SW), p - 1.0, p)
        q = (w_tok * p).astype(BF)
        q_s[:, cols] = q
        gw_ref[:, cols] += dot_tn(z, q)
    dz = dot_nt(q_s[...], w_ref[...])
    store_packed(dz_ref, dz, TB)
    if has_acc:
        @pl.when(pl.program_id(0) == N_DEV - 1)
        def _():
            for d in range(N_DEV):
                for c in range(VLOC // LANE):
                    pk_ref[d, c * Q:(c + 1) * Q, :] = gw_ref[Q * d:Q * d + Q, c * LANE:(c + 1) * LANE]


def head_pass2(z_all, w, tok, res, e, ms, acc):
    CHUNK_TOK = tok.shape[1]
    TB = CHUNK_TOK // N_DEV
    ZROWS = packed_rows(TB)
    in_specs = [
        rows_spec(1, ZROWS, LANE),
        whole(DIM, VLOC),
        lanes_spec(8, TB),
        lanes_spec(8, TB),
        rows_spec(TB, VLOC),
        rows_spec(TB, LANE),
    ]
    args = [z_all, w, tok, res, e, ms]
    g_shape = (DIM, VLOC) if acc is None else (N_DEV, GROWS, LANE)
    if acc is not None:
        in_specs.append(pl.BlockSpec((DIM, VLOC), lambda i: (0, 0), pipeline_mode=pl.Buffered(1)))
        args.append(acc)
    return pl.pallas_call(
        functools.partial(pass2_body, acc is not None),
        grid=(N_DEV,),
        in_specs=in_specs,
        out_specs=[
            rows_spec(1, ZROWS, LANE),
            pl.BlockSpec(g_shape, lambda i: tuple(0 * d for d in g_shape), pipeline_mode=pl.Buffered(1)),
        ],
        out_shape=[
            jax.ShapeDtypeStruct((N_DEV, ZROWS, LANE), F32),
            jax.ShapeDtypeStruct(g_shape, F32),
        ],
        scratch_shapes=[pltpu.VMEM((TB, DIM), BF), pltpu.VMEM((TB, VLOC), BF)] + ([] if acc is None else [pltpu.VMEM((DIM, VLOC), F32)]),
        compiler_params=pltpu.CompilerParams(vmem_limit_bytes=VMEM_LIMIT),
        cost_estimate=pl.CostEstimate(flops=4 * CHUNK_TOK * DIM * VLOC, bytes_accessed=4 * CHUNK_TOK * VLOC, transcendentals=0),
        name='head_pass2',
    )(*args)


def bwd_body(top, off, masks, n_in, *refs):
    h_ref, p_ref = refs[:2]
    if top:
        t_ref, d0_ref, d1_ref = refs[2:5]
    else:
        g_ref = refs[2]
    go_ref, buf_ref = refs[n_in:n_in + 2]
    scratch = refs[n_in + 2:]
    moves = []
    if masks:
        me = lax.axis_index(AXIS)
        pos = [me // w % 2 for w in (1, 2, 4, 8)]
        gp_ref = refs[n_in - 1 if top else n_in - 2]
        ga_ref, *scratch = scratch
        *scratch, send, recv, local = scratch
        barrier = pltpu.get_barrier_semaphore()
        mates = [me + sum(2**b * (1 - 2 * pos[b]) for b in range(4) if m >> b & 1) for m in masks]
        for j in mates:
            pl.semaphore_signal(barrier, inc=1, device_id=(j,), device_id_type=MESH)
        pl.semaphore_wait(barrier, len(masks))
        for i, j in enumerate(mates):
            moves.append(pltpu.make_async_remote_copy(
                src_ref=gp_ref.at[j], dst_ref=ga_ref.at[me], send_sem=send.at[i], recv_sem=recv.at[i],
                device_id=(j,), device_id_type=MESH))
        if top:
            moves.append(pltpu.make_async_copy(gp_ref.at[me], ga_ref.at[me], local))
        for move in moves:
            move.start()
    wg_ref, wu_ref, wd_ref, n_s, k_s, a_s, du_s, dv_s, pk_s, sem = scratch
    unpack_weights(p_ref, 0, wg_ref, wu_ref, wd_ref)

    for i, (lo, tb) in enumerate(SPLITS):
        rows = slice(lo, lo + tb)
        h = h_ref[rows, :].astype(F32)
        r = inv_rms_of(h)
        n = (h * r).astype(BF)
        if top:
            g = norm_grad(t_ref[rows, :].astype(F32), unpack_rows((d0_ref, d1_ref)[i], tb))
        else:
            g = g_ref[rows, :]
        k = g.astype(BF)
        u = dot_nn(n, wg_ref[...])
        v = dot_nn(n, wu_ref[...])
        e = dot_nt(k, wd_ref[...])
        sg = jax.nn.sigmoid(u)
        us = u * sg
        a_s[rows, :] = (us * v).astype(BF)
        du = (e * v * sg * (1.0 + u * (1.0 - sg))).astype(BF)
        dv = (e * us).astype(BF)
        n_s[rows, :] = n
        k_s[rows, :] = k
        du_s[rows, :] = du
        dv_s[rows, :] = dv
        dn = dot_nt(du, wg_ref[...]) + dot_nt(dv, wu_ref[...])
        go_ref[rows, :] = (g + r * dn - h * (r * r * r) * jnp.mean(h * dn, axis=-1, keepdims=True)).astype(go_ref.dtype)

    n = n_s[...]
    k = k_s[...]
    for c in range(6):
        gg = dot_tn(n, du_s[:, c * 256:(c + 1) * 256])
        gu = dot_tn(n, dv_s[:, c * 256:(c + 1) * 256])
        for j in range(2):
            base = (2 * c + j) * Q2
            for d in range(N_DEV):
                pk_s[d, base:base + Q, :] = gg[Q * d:Q * d + Q, j * LANE:(j + 1) * LANE]
                pk_s[d, base + Q:base + Q2, :] = gu[Q * d:Q * d + Q, j * LANE:(j + 1) * LANE]
    copy_a = pltpu.make_async_copy(pk_s.at[:, pl.ds(0, A0), :], buf_ref.at[:, pl.ds(off, A0), :], sem.at[0])
    copy_a.start()
    for c in range(4):
        gd = dot_tn(a_s[:, c * 384:(c + 1) * 384], k)
        for j in range(4):
            d = c * 4 + j
            x = gd[PD * j:PD * j + PD, :]
            for b in range(4):
                pk_s[d, A0 + PD * b:A0 + PD * b + PD, :] = x[:, LANE * b:LANE * b + LANE]
            pk_s[d, TL0:1296, :] = jnp.concatenate([x[:PH, D4:], x[PH:, D4:]], axis=1)
    copy_b = pltpu.make_async_copy(pk_s.at[:, pl.ds(A0, 432), :], buf_ref.at[:, pl.ds(off + A0, 432), :], sem.at[1])
    copy_b.start()
    copy_a.wait()
    copy_b.wait()
    for move in moves:
        move.wait()


def block_backward(h, packs, wslot, g_args, buf, slot, slots, out_dtype, masks=(), moved=(), cid=None):
    top = len(g_args) == 3
    args = [h, packs, *g_args]
    in_specs = [whole(TOK, DIM), pl.BlockSpec((N_DEV, 1, PROWS, LANE), lambda i: (0, wslot, 0, 0))]
    in_specs += [whole(*x.shape) for x in g_args]
    out_specs = [whole(TOK, DIM), HB]
    out_shape = [jax.ShapeDtypeStruct((TOK, DIM), out_dtype), jax.ShapeDtypeStruct((N_DEV, slots * PROWS, LANE), F32)]
    scratch = W_SCRATCH + [
        pltpu.VMEM((TOK, DIM), BF), pltpu.VMEM((TOK, DIM), BF), pltpu.VMEM((TOK, FFN), BF),
        pltpu.VMEM((TOK, FFN), BF), pltpu.VMEM((TOK, FFN), BF), pltpu.VMEM((N_DEV, PROWS, LANE), F32),
        pltpu.SemaphoreType.DMA((2,)),
    ]
    aliases = {}
    if buf is not None:
        aliases[len(args)] = 1
        args.append(buf)
        in_specs.append(HB)
    if masks:
        sems = pltpu.SemaphoreType.DMA((len(masks),))
        scratch += [sems, sems, pltpu.SemaphoreType.DMA]
        if len(moved) == 2:
            aliases[len(args) + 1] = 2
        args += moved
        in_specs += [HB] * len(moved)
        out_specs.append(HB)
        out_shape.append(jax.ShapeDtypeStruct(moved[0].shape, F32))
    return pl.pallas_call(
        functools.partial(bwd_body, top, slot * PROWS, masks, len(args)),
        grid=(1,),
        in_specs=in_specs,
        out_specs=out_specs,
        out_shape=out_shape,
        scratch_shapes=scratch,
        input_output_aliases=aliases,
        compiler_params=pltpu.CompilerParams(vmem_limit_bytes=VMEM_LIMIT, collective_id=cid, has_side_effects=bool(masks)),
        cost_estimate=pl.CostEstimate(flops=16 * TOK * DIM * FFN, bytes_accessed=24 * 2**20, transcendentals=TOK * FFN),
        name='block_backward',
    )(*args)


def head_unpack_body(p_ref, o_ref):
    for c in range(VLOC // LANE):
        o_ref[:, c * LANE:(c + 1) * LANE] = p_ref[0, c * Q:(c + 1) * Q, :]


def unpack_head(p):
    return pl.pallas_call(
        head_unpack_body,
        grid=(N_DEV,),
        in_specs=[rows_spec(1, GROWS, LANE)],
        out_specs=lanes_spec(Q, VLOC),
        out_shape=jax.ShapeDtypeStruct((Q, VOCAB), F32),
        name='unpack_head',
    )(p)


def cube_body(pieces, x_ref, o_ref, own, r0, r1, r2, r3, send, recv, local):
    me = lax.axis_index(AXIS)
    pos = [me // 8, me // 4 % 2, me // 2 % 2, me % 2]
    weight = (8, 4, 2, 1)
    mate = [me + w * (1 - 2 * p) for w, p in zip(weight, pos)]
    sem = pltpu.get_barrier_semaphore()
    for j in mate:
        pl.semaphore_signal(sem, inc=1, device_id=(j,), device_id_type=MESH)
    pl.semaphore_wait(sem, 4)
    core = pos[3]
    size = o_ref.shape[0] // (3 * pieces)
    units = [(k, (k + 3 * p) * size) for p in range(pieces) for k in range(3)]

    def pick(ref, k, stage, rows, flip):
        index = [slice(None)] * 3
        for j in range(stage):
            d = (k + j) % 3
            index[d] = pos[d]
        d = (k + stage) % 3
        index[d] = 1 - pos[d] if flip else pos[d]
        return ref.at[(*index, rows)]

    def landing(k, stage, rows):
        return (r1.at[:, :, rows], r2.at[:, rows], r3.at[rows])[stage]

    def first(u):
        k, base = units[u]
        rows = pl.ds(base, size)
        out = pltpu.make_async_remote_copy(
            src_ref=x_ref.at[:, :, :, 1 - core, rows], dst_ref=r0.at[:, :, :, rows], send_sem=send.at[0, u],
            recv_sem=recv.at[0, u], device_id=(mate[3],), device_id_type=MESH)
        return out, pltpu.make_async_copy(x_ref.at[:, :, :, core, rows], own.at[:, :, :, rows], local.at[u])

    def later(u, stage):
        k, base = units[u]
        rows = pl.ds(base, size)
        return pltpu.make_async_remote_copy(
            src_ref=pick(own, k, stage, rows, True), dst_ref=landing(k, stage, rows), send_sem=send.at[stage + 1, u],
            recv_sem=recv.at[stage + 1, u], device_id=(mate[(k + stage) % 3],), device_id_type=MESH)

    def add(dst, src):
        step = PH

        def body(i, carry):
            rows = pl.ds(pl.multiple_of(i * step, step), step)
            lead = (slice(None),) * (len(dst.shape) - 2)
            dst[(*lead, rows)] += src[(*lead, rows)]
            return carry

        lax.fori_loop(0, size // step, body, 0)

    many = range(len(units))
    for u in many:
        for copy in first(u):
            copy.start()
    for stage in range(4):
        for u in many:
            k, base = units[u]
            rows = pl.ds(base, size)
            if stage == 0:
                out, loc = first(u)
                loc.wait()
                out.wait_recv()
                add(own.at[:, :, :, rows], r0.at[:, :, :, rows])
            else:
                later(u, stage - 1).wait_recv()
                add(pick(own, k, stage - 1, rows, False), landing(k, stage - 1, rows))
            if stage < 3:
                if u > 0:
                    later(u - 1, stage).start()
                if u == many[-1]:
                    later(u, stage).start()
            else:
                o_ref[rows, :] = own[(*pos[:3], rows)]
    for u in many:
        first(u)[0].wait_send()
        for stage in range(3):
            later(u, stage).wait_send()


def cube_reduce_scatter(x, pieces, cid):
    rows = x.shape[1]
    units = 3 * pieces
    return pl.pallas_call(
        functools.partial(cube_body, pieces),
        in_specs=[HB],
        out_specs=VM,
        out_shape=jax.ShapeDtypeStruct((rows, LANE), F32),
        scratch_shapes=[
            pltpu.VMEM((2, 2, 2, rows, LANE), F32), pltpu.VMEM((2, 2, 2, rows, LANE), F32), pltpu.VMEM((2, 2, rows, LANE), F32),
            pltpu.VMEM((2, rows, LANE), F32), pltpu.VMEM((rows, LANE), F32),
            pltpu.SemaphoreType.DMA((4, units)), pltpu.SemaphoreType.DMA((4, units)), pltpu.SemaphoreType.DMA((units,)),
        ],
        compiler_params=pltpu.CompilerParams(collective_id=cid, has_side_effects=True, vmem_limit_bytes=VMEM_LIMIT),
        cost_estimate=pl.CostEstimate(flops=50 * 10**9, bytes_accessed=2**20, transcendentals=0),
        name='cube_reduce_scatter',
    )(x.reshape(2, 2, 2, 2, rows, LANE))


def unpack_body(has_prev, p_ref, *refs):
    gg_ref, gu_ref, gd_ref = refs[3:] if has_prev else refs
    for c in range(12):
        gg_ref[0, :, c * LANE:(c + 1) * LANE] = p_ref[c * Q2:c * Q2 + Q, :]
        gu_ref[0, :, c * LANE:(c + 1) * LANE] = p_ref[c * Q2 + Q:c * Q2 + Q2, :]
    for b in range(4):
        gd_ref[0, :, b * LANE:(b + 1) * LANE] = p_ref[A0 + PD * b:A0 + PD * b + PD, :]
    tail = p_ref[TL0:1296, :]
    gd_ref[0, 0:PH, D4:DIM] = tail[:, :HL]
    gd_ref[0, PH:PD, D4:DIM] = tail[:, HL:]


def unpack_grads(packed, group, prev):
    prev = list(prev or ())
    back = lambda i: (group[0] - i, 0, 0)
    return pl.pallas_call(
        functools.partial(unpack_body, bool(prev)),
        grid=(len(group),),
        in_specs=[rows_spec(PROWS, LANE)] + [HB] * len(prev),
        out_specs=[
            pl.BlockSpec((1, Q, FFN), back),
            pl.BlockSpec((1, Q, FFN), back),
            pl.BlockSpec((1, PD, DIM), back),
        ],
        out_shape=[
            jax.ShapeDtypeStruct((LAYERS, Q, FFN), F32),
            jax.ShapeDtypeStruct((LAYERS, Q, FFN), F32),
            jax.ShapeDtypeStruct((LAYERS, PD, DIM), F32),
        ],
        input_output_aliases={1 + i: i for i in range(len(prev))},
        name='unpack_grads',
    )(packed, *prev)


def pack_body(wg_ref, wu_ref, wd_ref, p_ref):
    for c in range(12):
        p_ref[0, c * Q2:c * Q2 + Q, :] = wg_ref[0, :, c * LANE:(c + 1) * LANE]
        p_ref[0, c * Q2 + Q:c * Q2 + Q2, :] = wu_ref[0, :, c * LANE:(c + 1) * LANE]
    for b in range(4):
        p_ref[0, A0 + PD * b:A0 + PD * b + PD, :] = wd_ref[0, :, b * LANE:(b + 1) * LANE]
    p_ref[0, TL0:1296, :] = jnp.concatenate([wd_ref[0, 0:PH, D4:DIM], wd_ref[0, PH:PD, D4:DIM]], axis=1)


def pack_weights(wg, wu, wd):
    return pl.pallas_call(
        pack_body,
        grid=(LAYERS,),
        in_specs=[
            rows_spec(1, Q, FFN),
            rows_spec(1, Q, FFN),
            rows_spec(1, PD, DIM),
        ],
        out_specs=rows_spec(1, PROWS, LANE),
        out_shape=jax.ShapeDtypeStruct((LAYERS, PROWS, LANE), BF),
        name='pack_weights',
    )(wg, wu, wd)


def unpack_weights(p_ref, slot, wg_s, wu_s, wd_s):
    for d in range(N_DEV):
        for c in range(12):
            cols = slice(c * LANE, (c + 1) * LANE)
            wg_s[Q * d:Q * d + Q, cols] = p_ref[d, slot, c * Q2:c * Q2 + Q, :]
            wu_s[Q * d:Q * d + Q, cols] = p_ref[d, slot, c * Q2 + Q:c * Q2 + Q2, :]
        for b in range(4):
            wd_s[PD * d:PD * d + PD, LANE * b:LANE * b + LANE] = p_ref[d, slot, A0 + PD * b:A0 + PD * b + PD, :]
        tail = p_ref[d, slot, TL0:1296, :]
        wd_s[PD * d:PD * d + PH, D4:DIM] = tail[:, :HL]
        wd_s[PD * d + PH:PD * d + PD, D4:DIM] = tail[:, HL:]


GROUPS = ((4, 3), (2, 1, 0))


def solution(mesh):
    def device_step(hidden, w_gate, w_up, w_down, w_out, targets, loss_mask):
        me = lax.axis_index(AXIS)
        gather = functools.partial(lax.all_gather, axis_name=AXIS)
        barrier = lax.optimization_barrier
        lab = jnp.concatenate([targets.astype(F32)[None], loss_mask.astype(F32)[None], jnp.zeros((6, TOK), F32)], axis=0)
        packs = pack_weights(w_gate, w_up, w_down)
        packs, lab = barrier((packs, lab))
        pack_top = gather(packs[4:])
        lab, w_vocab = start_exchange(lab, w_out)
        pack_top, w_vocab, lab = barrier((pack_top, w_vocab, lab))
        w_vocab = w_vocab.reshape(DIM, VLOC)
        t, *z_packed = top_forward(hidden[4], pack_top)

        mask = lab[:, 1, :]
        w_tok = mask / jnp.sum(mask)
        tgt = lab[:, 0, :] - (me * VLOC).astype(F32)
        w_own = lax.dynamic_slice(w_tok, (me, 0), (1, TOK))

        z_all = [lax.all_gather(z, AXIS, tiled=True) for z in z_packed]
        rest = gather(packs[:4])
        acc, loss, dz_own = None, jnp.zeros((), F32), []
        for c, (lo, tb) in enumerate(SPLITS):
            sl = slice(lo, lo + tb)
            CHUNK_TOK = tb * N_DEV
            zero = jnp.zeros((6, CHUNK_TOK), F32)
            tok = jnp.concatenate([tgt[:, sl].reshape(1, CHUNK_TOK), w_tok[:, sl].reshape(1, CHUNK_TOK), zero], axis=0)
            if c == 1:
                tok, acc, rest = barrier((tok, acc, rest))
            e, ms, st = head_pass1(z_all[c], w_vocab, tok)
            res = exchange_stats(st, w_own[:, sl], 2 + c)
            loss = loss + jnp.sum(res[2])
            dz, acc = head_pass2(z_all[c], w_vocab, tok, res, e, ms, acc)
            if c == 1:
                dz, dz_own[0] = barrier((dz, dz_own[0]))
                dz_own.append(cube_reduce_scatter(dz, 2, 4))
            else:
                dz_own.append(lax.psum_scatter(dz, AXIS, scatter_dimension=0, tiled=False))
        g_args = [t, *dz_own]
        bufs, moved = [], [acc]
        for group in GROUPS:
            buf = None
            for i, l in enumerate(group):
                pk, ws = (pack_top, 0) if l == 4 else (rest, l)
                args = (hidden[l], pk, ws, g_args, buf, i, len(group), BF if l == 0 else F32)
                if l > 2:
                    g, buf, got = block_backward(*args, tuple(range(2, 16, 2) if l == 4 else range(1, 16, 2)), moved, l + 3)
                    moved.append(got)
                else:
                    g, buf = block_backward(*args)
                g_args = [g]
            bufs.append(buf)
        grad_out = unpack_head(moved[2])
        red = lax.psum_scatter(bufs[0], AXIS, scatter_dimension=0, tiled=False)
        bufs[1], grad_out = barrier((bufs[1], grad_out))
        red_low = cube_reduce_scatter(bufs[1], 3, 5)
        red, red_low = barrier((red, red_low))
        outs = unpack_grads(red, GROUPS[0], None)
        grad_gate, grad_up, grad_down = unpack_grads(red_low, GROUPS[1], outs)
        return grad_gate, grad_up, grad_down, grad_out, g, loss

    stacked = P(None, AXIS, None)
    row = P(AXIS, None)
    return jax.shard_map(device_step, mesh=mesh, in_specs=(stacked, stacked, stacked, stacked, row, P(AXIS), P(AXIS)), out_specs=(stacked, stacked, stacked, row, row, P()), check_vma=False)
```

```python
import functools

import jax
import jax.numpy as jnp
from jax import lax
from jax.experimental import pallas as pl
from jax.experimental.pallas import tpu as pltpu
from jax.sharding import PartitionSpec as P

EPS = 1e-5
AXIS = 'fsdp'
N_DEV = 16
LAYERS = 5
TOK = 1024
DIM = 576
FFN = 1536
VOCAB = 49152
VLOC = VOCAB // N_DEV
TOKENS = TOK * N_DEV
SPLITS = ((0, 640), (640, 384))
STRIPS = 4
SW = VLOC // STRIPS
PROWS = 1296
BF = jnp.bfloat16
F32 = jnp.float32
MESH = pl.DeviceIdType.MESH
LANE = 128
D4 = 4 * LANE
HL = LANE // 2
Q = DIM // N_DEV
Q2 = 2 * Q
PD = FFN // N_DEV
PH = PD // 2
A0 = 12 * Q2
GROWS = VLOC // LANE * Q
TL0 = A0 + 4 * PD
VMEM_LIMIT = 62 * 1024 * 1024


def whole(*shape):
    return pl.BlockSpec(shape, lambda i: tuple(0 * d for d in shape))


def rows_spec(*shape):
    rest = shape[1:]
    return pl.BlockSpec(shape, lambda i: (i, *(0 * d for d in rest)))


def lanes_spec(*shape):
    return pl.BlockSpec(shape, lambda i: (0, i))


VM = pl.BlockSpec(memory_space=pltpu.VMEM)
HB = pl.BlockSpec(memory_space=pl.ANY)


def dot_nn(a, b):
    return lax.dot_general(a, b, (((1,), (0,)), ((), ())), preferred_element_type=F32)


def dot_nt(a, b):
    return lax.dot_general(a, b, (((1,), (1,)), ((), ())), preferred_element_type=F32)


def dot_tn(a, b):
    return lax.dot_general(a, b, (((0,), (0,)), ((), ())), preferred_element_type=F32)


def inv_rms_of(x):
    return lax.rsqrt(jnp.mean(x * x, axis=-1, keepdims=True) + EPS)


def norm_grad(x, e):
    r = inv_rms_of(x)
    return r * e - x * (r * r * r) * jnp.mean(x * e, axis=-1, keepdims=True)


def store_packed(ref, val, rows):
    half = rows // 2
    for c in range(4):
        ref[0, c * rows:(c + 1) * rows, :] = val[:, c * LANE:(c + 1) * LANE]
    ref[0, 4 * rows:4 * rows + half, :] = jnp.concatenate([val[:half, D4:], val[half:, D4:]], axis=1)


def load_packed(dst, ref, rows):
    half = rows // 2
    for c in range(4):
        dst[:, c * LANE:(c + 1) * LANE] = ref[0, c * rows:(c + 1) * rows, :]
    tail = ref[0, 4 * rows:4 * rows + half, :]
    dst[0:half, D4:DIM] = tail[:, :HL]
    dst[half:rows, D4:DIM] = tail[:, HL:]


def unpack_rows(p, rows):
    half = rows // 2
    tail = p[4 * rows:]
    tail = jnp.concatenate([tail[:, :HL], tail[:, HL:]], axis=0)
    return jnp.concatenate([p[c * rows:(c + 1) * rows] for c in range(4)] + [tail], axis=1)


W_SCRATCH = [pltpu.VMEM((DIM, FFN), BF), pltpu.VMEM((DIM, FFN), BF), pltpu.VMEM((FFN, DIM), BF)]


def fwd_body(h_ref, p_ref, t_ref, z0_ref, z1_ref, wg_ref, wu_ref, wd_ref):
    unpack_weights(p_ref, 0, wg_ref, wu_ref, wd_ref)
    for (off, tb), z_ref in zip(SPLITS, (z0_ref, z1_ref)):
        rows = slice(off, off + tb)
        h = h_ref[rows, :].astype(F32)
        n = (h * inv_rms_of(h)).astype(BF)
        u = dot_nn(n, wg_ref[...])
        v = dot_nn(n, wu_ref[...])
        a = (u * jax.nn.sigmoid(u) * v).astype(BF)
        t = (h + dot_nn(a, wd_ref[...])).astype(BF)
        t_ref[rows, :] = t
        t = t.astype(F32)
        store_packed(z_ref, (t * inv_rms_of(t)).astype(BF), tb)


def packed_rows(tb):
    return tb * 9 // 2


def top_forward(h, packs):
    zs = [(1, packed_rows(tb), LANE) for _, tb in SPLITS]
    return pl.pallas_call(
        fwd_body,
        grid=(1,),
        in_specs=[whole(TOK, DIM), whole(N_DEV, 1, PROWS, LANE)],
        out_specs=[whole(TOK, DIM)] + [whole(*z) for z in zs],
        out_shape=[jax.ShapeDtypeStruct((TOK, DIM), BF)] + [jax.ShapeDtypeStruct(z, BF) for z in zs],
        scratch_shapes=W_SCRATCH,
        compiler_params=pltpu.CompilerParams(vmem_limit_bytes=VMEM_LIMIT),
        cost_estimate=pl.CostEstimate(flops=6 * TOK * DIM * FFN, bytes_accessed=10 * 2**20, transcendentals=TOK * FFN),
        name='top_forward',
    )(h, packs)


def peers_barrier(me):
    sem = pltpu.get_barrier_semaphore()
    for off in range(1, N_DEV):
        pl.semaphore_signal(sem, inc=1, device_id=(lax.rem(me + off, N_DEV),), device_id_type=MESH)
    pl.semaphore_wait(sem, N_DEV - 1)


def all_send(me, src_of, dst, send_sem, recv_sem):
    copies = []
    for off in range(1, N_DEV):
        to = lax.rem(me + off, N_DEV)
        copy = pltpu.make_async_remote_copy(
            src_ref=src_of(to), dst_ref=dst.at[me], send_sem=send_sem.at[off], recv_sem=recv_sem.at[me],
            device_id=(to,), device_id_type=MESH)
        copy.start()
        copies.append(copy)
    return copies


def all_wait(me, src_of, dst, send_sem, recv_sem):
    for off in range(1, N_DEV):
        frm = lax.rem(me + N_DEV - off, N_DEV)
        copy = pltpu.make_async_remote_copy(
            src_ref=src_of(frm), dst_ref=dst.at[frm], send_sem=send_sem.at[off], recv_sem=recv_sem.at[frm],
            device_id=(frm,), device_id_type=MESH)
        copy.wait_recv()


def start_body(x_ref, w_ref, o_ref, wo_ref, buf, send_sem, recv_sem, send_w, recv_w, local):
    me = lax.axis_index(AXIS)
    peers_barrier(me)
    src = lambda j: x_ref
    part = lambda j: w_ref.at[:, pl.ds(pl.multiple_of(j * VLOC, VLOC), VLOC)]
    copies = all_send(me, src, buf, send_sem, recv_sem)
    copies += all_send(me, part, wo_ref, send_w, recv_w)
    mine = pltpu.make_async_copy(part(me), wo_ref.at[me], local)
    mine.start()
    all_wait(me, src, buf, send_sem, recv_sem)
    for j in range(N_DEV):
        o_ref[j] = jnp.where(me == j, x_ref[...], buf[j])
    all_wait(me, part, wo_ref, send_w, recv_w)
    mine.wait()
    for copy in copies:
        copy.wait_send()


def start_exchange(x, w):
    sems = pltpu.SemaphoreType.DMA((N_DEV,))
    return pl.pallas_call(
        start_body,
        in_specs=[VM, HB],
        out_specs=[VM, HB],
        out_shape=[jax.ShapeDtypeStruct((N_DEV, 8, TOK), F32), jax.ShapeDtypeStruct((N_DEV, Q, VLOC), BF)],
        scratch_shapes=[pltpu.VMEM((N_DEV, 8, TOK), F32), sems, sems, sems, sems, pltpu.SemaphoreType.DMA],
        compiler_params=pltpu.CompilerParams(collective_id=1, has_side_effects=True),
        cost_estimate=pl.CostEstimate(flops=50 * 10**9, bytes_accessed=2**20, transcendentals=0),
        name='start_exchange',
    )(x, w)


def stats_body(st_ref, w_ref, o_ref, buf1, own, buf2, send1, recv1, send2, recv2):
    me = lax.axis_index(AXIS)
    TB = w_ref.shape[1]
    peers_barrier(me)
    part = lambda j: st_ref.at[:, pl.ds(pl.multiple_of(j * TB, TB), TB)]
    copies = all_send(me, part, buf1, send1, recv1)
    all_wait(me, part, buf1, send1, recv1)
    mine = st_ref[:, pl.ds(pl.multiple_of(me * TB, TB), TB)]
    rows = [jnp.where(me == j, mine, buf1[j]) for j in range(N_DEV)]
    m = functools.reduce(jnp.maximum, [r[0:1] for r in rows])
    s = sum(r[1:2] * jnp.exp(r[0:1] - m) for r in rows)
    t = sum(r[2:3] for r in rows)
    own[...] = jnp.concatenate([m, 1.0 / s, w_ref[0:1, :] * (m + jnp.log(s) - t), jnp.zeros((5, TB), F32)], axis=0)
    src = lambda j: own
    copies += all_send(me, src, buf2, send2, recv2)
    all_wait(me, src, buf2, send2, recv2)
    for copy in copies:
        copy.wait_send()
    for j in range(N_DEV):
        o_ref[:, j * TB:(j + 1) * TB] = jnp.where(me == j, own[...], buf2[j])


def exchange_stats(st, w_own, cid):
    TB = w_own.shape[1]
    return pl.pallas_call(
        stats_body,
        in_specs=[VM, VM],
        out_specs=VM,
        out_shape=jax.ShapeDtypeStruct(st.shape, F32),
        scratch_shapes=[
            pltpu.VMEM((N_DEV, 8, TB), F32), pltpu.VMEM((8, TB), F32), pltpu.VMEM((N_DEV, 8, TB), F32),
            pltpu.SemaphoreType.DMA((N_DEV,)), pltpu.SemaphoreType.DMA((N_DEV,)),
            pltpu.SemaphoreType.DMA((N_DEV,)), pltpu.SemaphoreType.DMA((N_DEV,)),
        ],
        compiler_params=pltpu.CompilerParams(collective_id=cid, has_side_effects=True),
        cost_estimate=pl.CostEstimate(flops=2 * 10**9, bytes_accessed=2**20, transcendentals=0),
        name='exchange_stats',
    )(st, w_own)


def pass1_body(z_ref, w_ref, tok_ref, e_ref, ms_ref, st_ref, zt_ref, z_s):
    TB = z_s.shape[0]
    load_packed(z_s, z_ref, TB)
    z = z_s[...]
    zt_ref[...] = z.T
    tokc = jnp.concatenate([tok_ref[...], jnp.zeros((120, TB), F32)], axis=0).T
    tgt = tokc[:, 0:1]
    lane = lax.broadcasted_iota(jnp.int32, (TB, LANE), 1)
    ids = lax.broadcasted_iota(jnp.int32, (1, SW), 1).astype(F32)
    ms = jnp.zeros((TB, LANE), F32)
    tl = jnp.zeros((TB, 1), F32)
    m_list, s_list = [], []
    for s in range(STRIPS):
        l = dot_nn(z, w_ref[:, s * SW:(s + 1) * SW])
        m = jnp.max(l, axis=1, keepdims=True)
        e = jnp.exp(l - m)
        e_ref[:, s * SW:(s + 1) * SW] = e
        s_list.append(jnp.sum(e, axis=1, keepdims=True))
        m_list.append(m)
        tl = tl + jnp.sum(jnp.where(ids == tgt - float(s * SW), l, 0.0), axis=1, keepdims=True)
        ms = jnp.where(lane == s, m, ms)
    m_all = functools.reduce(jnp.maximum, m_list)
    s_all = sum(sv * jnp.exp(mv - m_all) for sv, mv in zip(s_list, m_list))
    ms_ref[...] = ms
    st = jnp.where(lane == 0, m_all, jnp.where(lane == 1, s_all, jnp.where(lane == 2, tl, 0.0)))
    st_ref[...] = st.T[0:8, :]


def head_pass1(z_all, w, tok):
    CHUNK_TOK = tok.shape[1]
    TB = CHUNK_TOK // N_DEV
    ZROWS = packed_rows(TB)
    return pl.pallas_call(
        pass1_body,
        grid=(N_DEV,),
        in_specs=[
            rows_spec(1, ZROWS, LANE),
            whole(DIM, VLOC),
            lanes_spec(8, TB),
        ],
        out_specs=[
            rows_spec(TB, VLOC),
            rows_spec(TB, LANE),
            lanes_spec(8, TB),
            lanes_spec(DIM, TB),
        ],
        out_shape=[
            jax.ShapeDtypeStruct((CHUNK_TOK, VLOC), F32),
            jax.ShapeDtypeStruct((CHUNK_TOK, LANE), F32),
            jax.ShapeDtypeStruct((8, CHUNK_TOK), F32),
            jax.ShapeDtypeStruct((DIM, CHUNK_TOK), BF),
        ],
        scratch_shapes=[pltpu.VMEM((TB, DIM), BF)],
        compiler_params=pltpu.CompilerParams(vmem_limit_bytes=VMEM_LIMIT),
        cost_estimate=pl.CostEstimate(flops=2 * CHUNK_TOK * DIM * VLOC, bytes_accessed=4 * CHUNK_TOK * VLOC, transcendentals=CHUNK_TOK * VLOC),
        name='head_pass1',
    )(z_all, w, tok)


def pass2_body(has_acc, *refs):
    if has_acc:
        z_ref, w_ref, tok_ref, res_ref, e_ref, ms_ref, acc_ref, dz_ref, pk_ref, q_s, gw_ref = refs
    else:
        z_ref, w_ref, tok_ref, res_ref, e_ref, ms_ref, dz_ref, gw_ref, q_s = refs
        acc_ref = None

    @pl.when(pl.program_id(0) == 0)
    def _():
        if has_acc:
            gw_ref[...] = acc_ref[...]
        else:
            gw_ref[...] = jnp.zeros_like(gw_ref)

    TB = q_s.shape[0]
    z = z_ref[...]
    tokc = jnp.concatenate([tok_ref[...], res_ref[...], jnp.zeros((112, TB), F32)], axis=0).T
    tgt, w_tok, m_glob, s_inv = (tokc[:, i:i + 1] for i in (0, 1, 8, 9))
    ids = lax.broadcasted_iota(jnp.int32, (1, SW), 1).astype(F32)
    for s in range(STRIPS):
        cols = slice(s * SW, (s + 1) * SW)
        scale = jnp.exp(ms_ref[:, s:s + 1] - m_glob) * s_inv
        p = e_ref[:, cols] * scale
        p = jnp.where(ids == tgt - float(s * SW), p - 1.0, p)
        q = (w_tok * p).astype(BF)
        q_s[:, cols] = q
        gw_ref[:, cols] += dot_nn(z, q)
    dz = dot_nt(q_s[...], w_ref[...])
    store_packed(dz_ref, dz, TB)
    if has_acc:
        @pl.when(pl.program_id(0) == N_DEV - 1)
        def _():
            for d in range(N_DEV):
                for c in range(VLOC // LANE):
                    pk_ref[d, c * Q:(c + 1) * Q, :] = gw_ref[Q * d:Q * d + Q, c * LANE:(c + 1) * LANE]


def head_pass2(z_all, w, tok, res, e, ms, acc):
    CHUNK_TOK = tok.shape[1]
    TB = CHUNK_TOK // N_DEV
    ZROWS = packed_rows(TB)
    in_specs = [
        lanes_spec(DIM, TB),
        whole(DIM, VLOC),
        lanes_spec(8, TB),
        lanes_spec(8, TB),
        rows_spec(TB, VLOC),
        rows_spec(TB, LANE),
    ]
    args = [z_all, w, tok, res, e, ms]
    g_shape = (DIM, VLOC) if acc is None else (N_DEV, GROWS, LANE)
    if acc is not None:
        in_specs.append(pl.BlockSpec((DIM, VLOC), lambda i: (0, 0), pipeline_mode=pl.Buffered(1)))
        args.append(acc)
    return pl.pallas_call(
        functools.partial(pass2_body, acc is not None),
        grid=(N_DEV,),
        in_specs=in_specs,
        out_specs=[
            rows_spec(1, ZROWS, LANE),
            pl.BlockSpec(g_shape, lambda i: tuple(0 * d for d in g_shape), pipeline_mode=pl.Buffered(1)),
        ],
        out_shape=[
            jax.ShapeDtypeStruct((N_DEV, ZROWS, LANE), F32),
            jax.ShapeDtypeStruct(g_shape, F32),
        ],
        scratch_shapes=[pltpu.VMEM((TB, VLOC), BF)] + ([] if acc is None else [pltpu.VMEM((DIM, VLOC), F32)]),
        compiler_params=pltpu.CompilerParams(vmem_limit_bytes=VMEM_LIMIT),
        cost_estimate=pl.CostEstimate(flops=4 * CHUNK_TOK * DIM * VLOC, bytes_accessed=4 * CHUNK_TOK * VLOC, transcendentals=0),
        name='head_pass2',
    )(*args)


def bwd_body(top, off, masks, n_in, *refs):
    h_ref, p_ref = refs[:2]
    if top:
        t_ref, d0_ref, d1_ref = refs[2:5]
    else:
        g_ref = refs[2]
    go_ref, buf_ref = refs[n_in:n_in + 2]
    scratch = refs[n_in + 2:]
    moves = []
    if masks:
        me = lax.axis_index(AXIS)
        pos = [me // w % 2 for w in (1, 2, 4, 8)]
        gp_ref = refs[n_in - 1 if top else n_in - 2]
        ga_ref, *scratch = scratch
        *scratch, send, recv, local = scratch
        barrier = pltpu.get_barrier_semaphore()
        mates = [me + sum(2**b * (1 - 2 * pos[b]) for b in range(4) if m >> b & 1) for m in masks]
        for j in mates:
            pl.semaphore_signal(barrier, inc=1, device_id=(j,), device_id_type=MESH)
        pl.semaphore_wait(barrier, len(masks))
        for i, j in enumerate(mates):
            moves.append(pltpu.make_async_remote_copy(
                src_ref=gp_ref.at[j], dst_ref=ga_ref.at[me], send_sem=send.at[i], recv_sem=recv.at[i],
                device_id=(j,), device_id_type=MESH))
        if top:
            moves.append(pltpu.make_async_copy(gp_ref.at[me], ga_ref.at[me], local))
        for move in moves:
            move.start()
    wg_ref, wu_ref, wd_ref, n_s, k_s, a_s, du_s, dv_s, pk_s, sem = scratch
    unpack_weights(p_ref, 0, wg_ref, wu_ref, wd_ref)

    for i, (lo, tb) in enumerate(SPLITS):
        rows = slice(lo, lo + tb)
        h = h_ref[rows, :].astype(F32)
        r = inv_rms_of(h)
        n = (h * r).astype(BF)
        if top:
            g = norm_grad(t_ref[rows, :].astype(F32), unpack_rows((d0_ref, d1_ref)[i], tb))
        else:
            g = g_ref[rows, :]
        k = g.astype(BF)
        u = dot_nn(n, wg_ref[...])
        v = dot_nn(n, wu_ref[...])
        e = dot_nt(k, wd_ref[...])
        sg = jax.nn.sigmoid(u)
        us = u * sg
        a_s[rows, :] = (us * v).astype(BF)
        du = (e * v * sg * (1.0 + u * (1.0 - sg))).astype(BF)
        dv = (e * us).astype(BF)
        n_s[rows, :] = n
        k_s[rows, :] = k
        du_s[rows, :] = du
        dv_s[rows, :] = dv
        dn = dot_nt(du, wg_ref[...]) + dot_nt(dv, wu_ref[...])
        go_ref[rows, :] = (g + r * dn - h * (r * r * r) * jnp.mean(h * dn, axis=-1, keepdims=True)).astype(go_ref.dtype)

    n = n_s[...]
    k = k_s[...]
    for c in range(6):
        gg = dot_tn(n, du_s[:, c * 256:(c + 1) * 256])
        gu = dot_tn(n, dv_s[:, c * 256:(c + 1) * 256])
        for j in range(2):
            base = (2 * c + j) * Q2
            for d in range(N_DEV):
                pk_s[d, base:base + Q, :] = gg[Q * d:Q * d + Q, j * LANE:(j + 1) * LANE]
                pk_s[d, base + Q:base + Q2, :] = gu[Q * d:Q * d + Q, j * LANE:(j + 1) * LANE]
    copy_a = pltpu.make_async_copy(pk_s.at[:, pl.ds(0, A0), :], buf_ref.at[:, pl.ds(off, A0), :], sem.at[0])
    copy_a.start()
    for c in range(4):
        gd = dot_tn(a_s[:, c * 384:(c + 1) * 384], k)
        for j in range(4):
            d = c * 4 + j
            x = gd[PD * j:PD * j + PD, :]
            for b in range(4):
                pk_s[d, A0 + PD * b:A0 + PD * b + PD, :] = x[:, LANE * b:LANE * b + LANE]
            pk_s[d, TL0:1296, :] = jnp.concatenate([x[:PH, D4:], x[PH:, D4:]], axis=1)
    copy_b = pltpu.make_async_copy(pk_s.at[:, pl.ds(A0, 432), :], buf_ref.at[:, pl.ds(off + A0, 432), :], sem.at[1])
    copy_b.start()
    copy_a.wait()
    copy_b.wait()
    for move in moves:
        move.wait()


def block_backward(h, packs, wslot, g_args, buf, slot, slots, out_dtype, masks=(), moved=(), cid=None):
    top = len(g_args) == 3
    args = [h, packs, *g_args]
    in_specs = [whole(TOK, DIM), pl.BlockSpec((N_DEV, 1, PROWS, LANE), lambda i: (0, wslot, 0, 0))]
    in_specs += [whole(*x.shape) for x in g_args]
    out_specs = [whole(TOK, DIM), HB]
    out_shape = [jax.ShapeDtypeStruct((TOK, DIM), out_dtype), jax.ShapeDtypeStruct((N_DEV, slots * PROWS, LANE), F32)]
    scratch = W_SCRATCH + [
        pltpu.VMEM((TOK, DIM), BF), pltpu.VMEM((TOK, DIM), BF), pltpu.VMEM((TOK, FFN), BF),
        pltpu.VMEM((TOK, FFN), BF), pltpu.VMEM((TOK, FFN), BF), pltpu.VMEM((N_DEV, PROWS, LANE), F32),
        pltpu.SemaphoreType.DMA((2,)),
    ]
    aliases = {}
    if buf is not None:
        aliases[len(args)] = 1
        args.append(buf)
        in_specs.append(HB)
    if masks:
        sems = pltpu.SemaphoreType.DMA((len(masks),))
        scratch += [sems, sems, pltpu.SemaphoreType.DMA]
        if len(moved) == 2:
            aliases[len(args) + 1] = 2
        args += moved
        in_specs += [HB] * len(moved)
        out_specs.append(HB)
        out_shape.append(jax.ShapeDtypeStruct(moved[0].shape, F32))
    return pl.pallas_call(
        functools.partial(bwd_body, top, slot * PROWS, masks, len(args)),
        grid=(1,),
        in_specs=in_specs,
        out_specs=out_specs,
        out_shape=out_shape,
        scratch_shapes=scratch,
        input_output_aliases=aliases,
        compiler_params=pltpu.CompilerParams(vmem_limit_bytes=VMEM_LIMIT, collective_id=cid, has_side_effects=bool(masks)),
        cost_estimate=pl.CostEstimate(flops=16 * TOK * DIM * FFN, bytes_accessed=24 * 2**20, transcendentals=TOK * FFN),
        name='block_backward',
    )(*args)


def head_unpack_body(p_ref, o_ref):
    for c in range(VLOC // LANE):
        o_ref[:, c * LANE:(c + 1) * LANE] = p_ref[0, c * Q:(c + 1) * Q, :]


def unpack_head(p):
    return pl.pallas_call(
        head_unpack_body,
        grid=(N_DEV,),
        in_specs=[rows_spec(1, GROWS, LANE)],
        out_specs=lanes_spec(Q, VLOC),
        out_shape=jax.ShapeDtypeStruct((Q, VOCAB), F32),
        name='unpack_head',
    )(p)


def cube_body(pieces, x_ref, o_ref, own, r0, r1, r2, r3, send, recv, local):
    me = lax.axis_index(AXIS)
    pos = [me // 8, me // 4 % 2, me // 2 % 2, me % 2]
    weight = (8, 4, 2, 1)
    mate = [me + w * (1 - 2 * p) for w, p in zip(weight, pos)]
    sem = pltpu.get_barrier_semaphore()
    for j in mate:
        pl.semaphore_signal(sem, inc=1, device_id=(j,), device_id_type=MESH)
    pl.semaphore_wait(sem, 4)
    core = pos[3]
    size = o_ref.shape[0] // (3 * pieces)
    units = [(k, (k + 3 * p) * size) for p in range(pieces) for k in range(3)]

    def pick(ref, k, stage, rows, flip):
        index = [slice(None)] * 3
        for j in range(stage):
            d = (k + j) % 3
            index[d] = pos[d]
        d = (k + stage) % 3
        index[d] = 1 - pos[d] if flip else pos[d]
        return ref.at[(*index, rows)]

    def landing(k, stage, rows):
        return (r1.at[:, :, rows], r2.at[:, rows], r3.at[rows])[stage]

    def first(u):
        k, base = units[u]
        rows = pl.ds(base, size)
        out = pltpu.make_async_remote_copy(
            src_ref=x_ref.at[:, :, :, 1 - core, rows], dst_ref=r0.at[:, :, :, rows], send_sem=send.at[0, u],
            recv_sem=recv.at[0, u], device_id=(mate[3],), device_id_type=MESH)
        return out, pltpu.make_async_copy(x_ref.at[:, :, :, core, rows], own.at[:, :, :, rows], local.at[u])

    def later(u, stage):
        k, base = units[u]
        rows = pl.ds(base, size)
        return pltpu.make_async_remote_copy(
            src_ref=pick(own, k, stage, rows, True), dst_ref=landing(k, stage, rows), send_sem=send.at[stage + 1, u],
            recv_sem=recv.at[stage + 1, u], device_id=(mate[(k + stage) % 3],), device_id_type=MESH)

    def add(dst, src):
        step = PH

        def body(i, carry):
            rows = pl.ds(pl.multiple_of(i * step, step), step)
            lead = (slice(None),) * (len(dst.shape) - 2)
            dst[(*lead, rows)] += src[(*lead, rows)]
            return carry

        lax.fori_loop(0, size // step, body, 0)

    many = range(len(units))
    for u in many:
        for copy in first(u):
            copy.start()
    for stage in range(4):
        for u in many:
            k, base = units[u]
            rows = pl.ds(base, size)
            if stage == 0:
                out, loc = first(u)
                loc.wait()
                out.wait_recv()
                add(own.at[:, :, :, rows], r0.at[:, :, :, rows])
            else:
                later(u, stage - 1).wait_recv()
                add(pick(own, k, stage - 1, rows, False), landing(k, stage - 1, rows))
            if stage < 3:
                if u > 0:
                    later(u - 1, stage).start()
                if u == many[-1]:
                    later(u, stage).start()
            else:
                o_ref[rows, :] = own[(*pos[:3], rows)]
    for u in many:
        first(u)[0].wait_send()
        for stage in range(3):
            later(u, stage).wait_send()


def cube_reduce_scatter(x, pieces, cid):
    rows = x.shape[1]
    units = 3 * pieces
    return pl.pallas_call(
        functools.partial(cube_body, pieces),
        in_specs=[HB],
        out_specs=VM,
        out_shape=jax.ShapeDtypeStruct((rows, LANE), F32),
        scratch_shapes=[
            pltpu.VMEM((2, 2, 2, rows, LANE), F32), pltpu.VMEM((2, 2, 2, rows, LANE), F32), pltpu.VMEM((2, 2, rows, LANE), F32),
            pltpu.VMEM((2, rows, LANE), F32), pltpu.VMEM((rows, LANE), F32),
            pltpu.SemaphoreType.DMA((4, units)), pltpu.SemaphoreType.DMA((4, units)), pltpu.SemaphoreType.DMA((units,)),
        ],
        compiler_params=pltpu.CompilerParams(collective_id=cid, has_side_effects=True, vmem_limit_bytes=VMEM_LIMIT),
        cost_estimate=pl.CostEstimate(flops=50 * 10**9, bytes_accessed=2**20, transcendentals=0),
        name='cube_reduce_scatter',
    )(x.reshape(2, 2, 2, 2, rows, LANE))


def unpack_body(has_prev, p_ref, *refs):
    gg_ref, gu_ref, gd_ref = refs[3:] if has_prev else refs
    for c in range(12):
        gg_ref[0, :, c * LANE:(c + 1) * LANE] = p_ref[c * Q2:c * Q2 + Q, :]
        gu_ref[0, :, c * LANE:(c + 1) * LANE] = p_ref[c * Q2 + Q:c * Q2 + Q2, :]
    for b in range(4):
        gd_ref[0, :, b * LANE:(b + 1) * LANE] = p_ref[A0 + PD * b:A0 + PD * b + PD, :]
    tail = p_ref[TL0:1296, :]
    gd_ref[0, 0:PH, D4:DIM] = tail[:, :HL]
    gd_ref[0, PH:PD, D4:DIM] = tail[:, HL:]


def unpack_grads(packed, group, prev):
    prev = list(prev or ())
    back = lambda i: (group[0] - i, 0, 0)
    return pl.pallas_call(
        functools.partial(unpack_body, bool(prev)),
        grid=(len(group),),
        in_specs=[rows_spec(PROWS, LANE)] + [HB] * len(prev),
        out_specs=[
            pl.BlockSpec((1, Q, FFN), back),
            pl.BlockSpec((1, Q, FFN), back),
            pl.BlockSpec((1, PD, DIM), back),
        ],
        out_shape=[
            jax.ShapeDtypeStruct((LAYERS, Q, FFN), F32),
            jax.ShapeDtypeStruct((LAYERS, Q, FFN), F32),
            jax.ShapeDtypeStruct((LAYERS, PD, DIM), F32),
        ],
        input_output_aliases={1 + i: i for i in range(len(prev))},
        name='unpack_grads',
    )(packed, *prev)


def pack_body(wg_ref, wu_ref, wd_ref, p_ref):
    for c in range(12):
        p_ref[0, c * Q2:c * Q2 + Q, :] = wg_ref[0, :, c * LANE:(c + 1) * LANE]
        p_ref[0, c * Q2 + Q:c * Q2 + Q2, :] = wu_ref[0, :, c * LANE:(c + 1) * LANE]
    for b in range(4):
        p_ref[0, A0 + PD * b:A0 + PD * b + PD, :] = wd_ref[0, :, b * LANE:(b + 1) * LANE]
    p_ref[0, TL0:1296, :] = jnp.concatenate([wd_ref[0, 0:PH, D4:DIM], wd_ref[0, PH:PD, D4:DIM]], axis=1)


def pack_weights(wg, wu, wd):
    return pl.pallas_call(
        pack_body,
        grid=(LAYERS,),
        in_specs=[
            rows_spec(1, Q, FFN),
            rows_spec(1, Q, FFN),
            rows_spec(1, PD, DIM),
        ],
        out_specs=rows_spec(1, PROWS, LANE),
        out_shape=jax.ShapeDtypeStruct((LAYERS, PROWS, LANE), BF),
        name='pack_weights',
    )(wg, wu, wd)


def unpack_weights(p_ref, slot, wg_s, wu_s, wd_s):
    for d in range(N_DEV):
        for c in range(12):
            cols = slice(c * LANE, (c + 1) * LANE)
            wg_s[Q * d:Q * d + Q, cols] = p_ref[d, slot, c * Q2:c * Q2 + Q, :]
            wu_s[Q * d:Q * d + Q, cols] = p_ref[d, slot, c * Q2 + Q:c * Q2 + Q2, :]
        for b in range(4):
            wd_s[PD * d:PD * d + PD, LANE * b:LANE * b + LANE] = p_ref[d, slot, A0 + PD * b:A0 + PD * b + PD, :]
        tail = p_ref[d, slot, TL0:1296, :]
        wd_s[PD * d:PD * d + PH, D4:DIM] = tail[:, :HL]
        wd_s[PD * d + PH:PD * d + PD, D4:DIM] = tail[:, HL:]


PEERS = ((1,), (3, 5, 9, 15), (2, 4, 8, 14), (7, 11, 13), (6, 10, 12))
GROUPS = ((4, 3), (2, 1, 0))


def solution(mesh):
    def device_step(hidden, w_gate, w_up, w_down, w_out, targets, loss_mask):
        me = lax.axis_index(AXIS)
        gather = functools.partial(lax.all_gather, axis_name=AXIS)
        barrier = lax.optimization_barrier
        lab = jnp.concatenate([targets.astype(F32)[None], loss_mask.astype(F32)[None], jnp.zeros((6, TOK), F32)], axis=0)
        packs = pack_weights(w_gate, w_up, w_down)
        packs, lab = barrier((packs, lab))
        pack_top = gather(packs[4:])
        lab, w_vocab = start_exchange(lab, w_out)
        pack_top, w_vocab, lab = barrier((pack_top, w_vocab, lab))
        w_vocab = w_vocab.reshape(DIM, VLOC)
        t, *z_packed = top_forward(hidden[4], pack_top)

        mask = lab[:, 1, :]
        w_tok = mask / jnp.sum(mask)
        tgt = lab[:, 0, :] - (me * VLOC).astype(F32)
        w_own = lax.dynamic_slice(w_tok, (me, 0), (1, TOK))

        z_all = [lax.all_gather(z, AXIS, tiled=True) for z in z_packed]
        rest = gather(packs[:4])
        acc, loss, dz_own = None, jnp.zeros((), F32), []
        for c, (lo, tb) in enumerate(SPLITS):
            sl = slice(lo, lo + tb)
            CHUNK_TOK = tb * N_DEV
            zero = jnp.zeros((6, CHUNK_TOK), F32)
            tok = jnp.concatenate([tgt[:, sl].reshape(1, CHUNK_TOK), w_tok[:, sl].reshape(1, CHUNK_TOK), zero], axis=0)
            if c == 1:
                tok, acc, rest = barrier((tok, acc, rest))
            e, ms, st, z_t = head_pass1(z_all[c], w_vocab, tok)
            res = exchange_stats(st, w_own[:, sl], 2 + c)
            loss = loss + jnp.sum(res[2])
            dz, acc = head_pass2(z_t, w_vocab, tok, res, e, ms, acc)
            if c == 1:
                dz, dz_own[0] = barrier((dz, dz_own[0]))
                dz_own.append(cube_reduce_scatter(dz, 2, 4))
            else:
                dz_own.append(lax.psum_scatter(dz, AXIS, scatter_dimension=0, tiled=False))
        g_args = [t, *dz_own]
        bufs, moved = [], [acc]
        for group in GROUPS:
            buf = None
            for i, l in enumerate(group):
                pk, ws = (pack_top, 0) if l == 4 else (rest, l)
                args = (hidden[l], pk, ws, g_args, buf, i, len(group), BF if l == 0 else F32)
                g, buf, got = block_backward(*args, PEERS[l], moved, l + 6)
                moved = [acc, got]
                g_args = [g]
            bufs.append(buf)
        grad_out = unpack_head(moved[1])
        red = lax.psum_scatter(bufs[0], AXIS, scatter_dimension=0, tiled=False)
        bufs[1], grad_out = barrier((bufs[1], grad_out))
        red_low = cube_reduce_scatter(bufs[1], 3, 5)
        red, red_low = barrier((red, red_low))
        outs = unpack_grads(red, GROUPS[0], None)
        grad_gate, grad_up, grad_down = unpack_grads(red_low, GROUPS[1], outs)
        return grad_gate, grad_up, grad_down, grad_out, g, loss

    stacked = P(None, AXIS, None)
    row = P(AXIS, None)
    return jax.shard_map(device_step, mesh=mesh, in_specs=(stacked, stacked, stacked, stacked, row, P(AXIS), P(AXIS)), out_specs=(stacked, stacked, stacked, row, row, P()), check_vma=False)
```

```python
import functools

import jax
import jax.numpy as jnp
from jax import lax
from jax.experimental import pallas as pl
from jax.experimental.pallas import tpu as pltpu
from jax.sharding import PartitionSpec as P

EPS = 1e-5
AXIS = 'fsdp'
N_DEV = 16
LAYERS = 5
TOK = 1024
DIM = 576
FFN = 1536
VOCAB = 49152
VLOC = VOCAB // N_DEV
TOKENS = TOK * N_DEV
SPLITS = ((0, 640), (640, 384))
STRIPS = 4
SW = VLOC // STRIPS
PROWS = 1296
BF = jnp.bfloat16
F32 = jnp.float32
MESH = pl.DeviceIdType.MESH
LANE = 128
D4 = 4 * LANE
HL = LANE // 2
Q = DIM // N_DEV
Q2 = 2 * Q
PD = FFN // N_DEV
PH = PD // 2
A0 = 12 * Q2
GROWS = VLOC // LANE * Q
TL0 = A0 + 4 * PD
VMEM_LIMIT = 62 * 1024 * 1024


def whole(*shape):
    return pl.BlockSpec(shape, lambda i: tuple(0 * d for d in shape))


def rows_spec(*shape):
    rest = shape[1:]
    return pl.BlockSpec(shape, lambda i: (i, *(0 * d for d in rest)))


def lanes_spec(*shape):
    return pl.BlockSpec(shape, lambda i: (0, i))


VM = pl.BlockSpec(memory_space=pltpu.VMEM)
HB = pl.BlockSpec(memory_space=pl.ANY)


def dot_nn(a, b):
    return lax.dot_general(a, b, (((1,), (0,)), ((), ())), preferred_element_type=F32)


def dot_nt(a, b):
    return lax.dot_general(a, b, (((1,), (1,)), ((), ())), preferred_element_type=F32)


def dot_tn(a, b):
    return lax.dot_general(a, b, (((0,), (0,)), ((), ())), preferred_element_type=F32)


def inv_rms_of(x):
    return lax.rsqrt(jnp.mean(x * x, axis=-1, keepdims=True) + EPS)


def norm_grad(x, e):
    r = inv_rms_of(x)
    return r * e - x * (r * r * r) * jnp.mean(x * e, axis=-1, keepdims=True)


def store_packed(ref, val, rows):
    half = rows // 2
    for c in range(4):
        ref[0, c * rows:(c + 1) * rows, :] = val[:, c * LANE:(c + 1) * LANE]
    ref[0, 4 * rows:4 * rows + half, :] = jnp.concatenate([val[:half, D4:], val[half:, D4:]], axis=1)


def load_packed(dst, ref, rows):
    half = rows // 2
    for c in range(4):
        dst[:, c * LANE:(c + 1) * LANE] = ref[0, c * rows:(c + 1) * rows, :]
    tail = ref[0, 4 * rows:4 * rows + half, :]
    dst[0:half, D4:DIM] = tail[:, :HL]
    dst[half:rows, D4:DIM] = tail[:, HL:]


def unpack_rows(p, rows):
    half = rows // 2
    tail = p[4 * rows:]
    tail = jnp.concatenate([tail[:, :HL], tail[:, HL:]], axis=0)
    return jnp.concatenate([p[c * rows:(c + 1) * rows] for c in range(4)] + [tail], axis=1)


W_SCRATCH = [pltpu.VMEM((DIM, FFN), BF), pltpu.VMEM((DIM, FFN), BF), pltpu.VMEM((FFN, DIM), BF)]


def fwd_body(h_ref, p_ref, t_ref, z0_ref, z1_ref, wg_ref, wu_ref, wd_ref):
    unpack_weights(p_ref, 0, wg_ref, wu_ref, wd_ref)
    for (off, tb), z_ref in zip(SPLITS, (z0_ref, z1_ref)):
        rows = slice(off, off + tb)
        h = h_ref[rows, :].astype(F32)
        n = (h * inv_rms_of(h)).astype(BF)
        u = dot_nn(n, wg_ref[...])
        v = dot_nn(n, wu_ref[...])
        a = (u * jax.nn.sigmoid(u) * v).astype(BF)
        t = (h + dot_nn(a, wd_ref[...])).astype(BF)
        t_ref[rows, :] = t
        t = t.astype(F32)
        store_packed(z_ref, (t * inv_rms_of(t)).astype(BF), tb)


def packed_rows(tb):
    return tb * 9 // 2


def top_forward(h, packs):
    zs = [(1, packed_rows(tb), LANE) for _, tb in SPLITS]
    return pl.pallas_call(
        fwd_body,
        grid=(1,),
        in_specs=[whole(TOK, DIM), whole(N_DEV, 1, PROWS, LANE)],
        out_specs=[whole(TOK, DIM)] + [whole(*z) for z in zs],
        out_shape=[jax.ShapeDtypeStruct((TOK, DIM), BF)] + [jax.ShapeDtypeStruct(z, BF) for z in zs],
        scratch_shapes=W_SCRATCH,
        compiler_params=pltpu.CompilerParams(vmem_limit_bytes=VMEM_LIMIT),
        cost_estimate=pl.CostEstimate(flops=6 * TOK * DIM * FFN, bytes_accessed=10 * 2**20, transcendentals=TOK * FFN),
        name='top_forward',
    )(h, packs)


def peers_barrier(me):
    sem = pltpu.get_barrier_semaphore()
    for off in range(1, N_DEV):
        pl.semaphore_signal(sem, inc=1, device_id=(lax.rem(me + off, N_DEV),), device_id_type=MESH)
    pl.semaphore_wait(sem, N_DEV - 1)


def all_send(me, src_of, dst, send_sem, recv_sem):
    copies = []
    for off in range(1, N_DEV):
        to = lax.rem(me + off, N_DEV)
        copy = pltpu.make_async_remote_copy(
            src_ref=src_of(to), dst_ref=dst.at[me], send_sem=send_sem.at[off], recv_sem=recv_sem.at[me],
            device_id=(to,), device_id_type=MESH)
        copy.start()
        copies.append(copy)
    return copies


def all_wait(me, src_of, dst, send_sem, recv_sem):
    for off in range(1, N_DEV):
        frm = lax.rem(me + N_DEV - off, N_DEV)
        copy = pltpu.make_async_remote_copy(
            src_ref=src_of(frm), dst_ref=dst.at[frm], send_sem=send_sem.at[off], recv_sem=recv_sem.at[frm],
            device_id=(frm,), device_id_type=MESH)
        copy.wait_recv()


def start_body(x_ref, w_ref, o_ref, wo_ref, buf, send_sem, recv_sem, send_w, recv_w, local):
    me = lax.axis_index(AXIS)
    peers_barrier(me)
    src = lambda j: x_ref
    part = lambda j: w_ref.at[:, pl.ds(pl.multiple_of(j * VLOC, VLOC), VLOC)]
    copies = all_send(me, src, buf, send_sem, recv_sem)
    copies += all_send(me, part, wo_ref, send_w, recv_w)
    mine = pltpu.make_async_copy(part(me), wo_ref.at[me], local)
    mine.start()
    all_wait(me, src, buf, send_sem, recv_sem)
    for j in range(N_DEV):
        o_ref[j] = jnp.where(me == j, x_ref[...], buf[j])
    all_wait(me, part, wo_ref, send_w, recv_w)
    mine.wait()
    for copy in copies:
        copy.wait_send()


def start_exchange(x, w):
    sems = pltpu.SemaphoreType.DMA((N_DEV,))
    return pl.pallas_call(
        start_body,
        in_specs=[VM, HB],
        out_specs=[VM, HB],
        out_shape=[jax.ShapeDtypeStruct((N_DEV, 8, TOK), F32), jax.ShapeDtypeStruct((N_DEV, Q, VLOC), BF)],
        scratch_shapes=[pltpu.VMEM((N_DEV, 8, TOK), F32), sems, sems, sems, sems, pltpu.SemaphoreType.DMA],
        compiler_params=pltpu.CompilerParams(collective_id=1, has_side_effects=True),
        cost_estimate=pl.CostEstimate(flops=50 * 10**9, bytes_accessed=2**20, transcendentals=0),
        name='start_exchange',
    )(x, w)


def stats_body(st_ref, w_ref, o_ref, buf1, own, buf2, send1, recv1, send2, recv2):
    me = lax.axis_index(AXIS)
    TB = w_ref.shape[1]
    peers_barrier(me)
    part = lambda j: st_ref.at[:, pl.ds(pl.multiple_of(j * TB, TB), TB)]
    copies = all_send(me, part, buf1, send1, recv1)
    all_wait(me, part, buf1, send1, recv1)
    mine = st_ref[:, pl.ds(pl.multiple_of(me * TB, TB), TB)]
    rows = [jnp.where(me == j, mine, buf1[j]) for j in range(N_DEV)]
    m = functools.reduce(jnp.maximum, [r[0:1] for r in rows])
    s = sum(r[1:2] * jnp.exp(r[0:1] - m) for r in rows)
    t = sum(r[2:3] for r in rows)
    own[...] = jnp.concatenate([m, 1.0 / s, w_ref[0:1, :] * (m + jnp.log(s) - t), jnp.zeros((5, TB), F32)], axis=0)
    src = lambda j: own
    copies += all_send(me, src, buf2, send2, recv2)
    all_wait(me, src, buf2, send2, recv2)
    for copy in copies:
        copy.wait_send()
    for j in range(N_DEV):
        o_ref[:, j * TB:(j + 1) * TB] = jnp.where(me == j, own[...], buf2[j])


def exchange_stats(st, w_own, cid):
    TB = w_own.shape[1]
    return pl.pallas_call(
        stats_body,
        in_specs=[VM, VM],
        out_specs=VM,
        out_shape=jax.ShapeDtypeStruct(st.shape, F32),
        scratch_shapes=[
            pltpu.VMEM((N_DEV, 8, TB), F32), pltpu.VMEM((8, TB), F32), pltpu.VMEM((N_DEV, 8, TB), F32),
            pltpu.SemaphoreType.DMA((N_DEV,)), pltpu.SemaphoreType.DMA((N_DEV,)),
            pltpu.SemaphoreType.DMA((N_DEV,)), pltpu.SemaphoreType.DMA((N_DEV,)),
        ],
        compiler_params=pltpu.CompilerParams(collective_id=cid, has_side_effects=True),
        cost_estimate=pl.CostEstimate(flops=2 * 10**9, bytes_accessed=2**20, transcendentals=0),
        name='exchange_stats',
    )(st, w_own)


def pass1_body(z_ref, w_ref, tok_ref, e_ref, ms_ref, st_ref, zt_ref, z_s):
    TB = z_s.shape[0]
    load_packed(z_s, z_ref, TB)
    z = z_s[...]
    zt_ref[...] = z.T
    tokc = jnp.concatenate([tok_ref[...], jnp.zeros((120, TB), F32)], axis=0).T
    tgt = tokc[:, 0:1]
    lane = lax.broadcasted_iota(jnp.int32, (TB, LANE), 1)
    ids = lax.broadcasted_iota(jnp.int32, (1, SW), 1).astype(F32)
    ms = jnp.zeros((TB, LANE), F32)
    tl = jnp.zeros((TB, 1), F32)
    m_list, s_list = [], []
    for s in range(STRIPS):
        l = dot_nn(z, w_ref[:, s * SW:(s + 1) * SW])
        m = jnp.max(l, axis=1, keepdims=True)
        e = jnp.exp(l - m)
        e_ref[:, s * SW:(s + 1) * SW] = e
        s_list.append(jnp.sum(e, axis=1, keepdims=True))
        m_list.append(m)
        tl = tl + jnp.sum(jnp.where(ids == tgt - float(s * SW), l, 0.0), axis=1, keepdims=True)
        ms = jnp.where(lane == s, m, ms)
    m_all = functools.reduce(jnp.maximum, m_list)
    s_all = sum(sv * jnp.exp(mv - m_all) for sv, mv in zip(s_list, m_list))
    ms_ref[...] = ms
    st = jnp.where(lane == 0, m_all, jnp.where(lane == 1, s_all, jnp.where(lane == 2, tl, 0.0)))
    st_ref[...] = st.T[0:8, :]


def head_pass1(z_all, w, tok):
    CHUNK_TOK = tok.shape[1]
    TB = CHUNK_TOK // N_DEV
    ZROWS = packed_rows(TB)
    return pl.pallas_call(
        pass1_body,
        grid=(N_DEV,),
        in_specs=[
            rows_spec(1, ZROWS, LANE),
            whole(DIM, VLOC),
            lanes_spec(8, TB),
        ],
        out_specs=[
            rows_spec(TB, VLOC),
            rows_spec(TB, LANE),
            lanes_spec(8, TB),
            lanes_spec(DIM, TB),
        ],
        out_shape=[
            jax.ShapeDtypeStruct((CHUNK_TOK, VLOC), F32),
            jax.ShapeDtypeStruct((CHUNK_TOK, LANE), F32),
            jax.ShapeDtypeStruct((8, CHUNK_TOK), F32),
            jax.ShapeDtypeStruct((DIM, CHUNK_TOK), BF),
        ],
        scratch_shapes=[pltpu.VMEM((TB, DIM), BF)],
        compiler_params=pltpu.CompilerParams(vmem_limit_bytes=VMEM_LIMIT),
        cost_estimate=pl.CostEstimate(flops=2 * CHUNK_TOK * DIM * VLOC, bytes_accessed=4 * CHUNK_TOK * VLOC, transcendentals=CHUNK_TOK * VLOC),
        name='head_pass1',
    )(z_all, w, tok)


def pass2_body(has_acc, *refs):
    if has_acc:
        z_ref, w_ref, tok_ref, res_ref, e_ref, ms_ref, acc_ref, dz_ref, pk_ref, q_s, gw_ref = refs
    else:
        z_ref, w_ref, tok_ref, res_ref, e_ref, ms_ref, dz_ref, gw_ref, q_s = refs
        acc_ref = None

    @pl.when(pl.program_id(0) == 0)
    def _():
        if has_acc:
            gw_ref[...] = acc_ref[...]
        else:
            gw_ref[...] = jnp.zeros_like(gw_ref)

    TB = q_s.shape[0]
    z = z_ref[...]
    tokc = jnp.concatenate([tok_ref[...], res_ref[...], jnp.zeros((112, TB), F32)], axis=0).T
    tgt, w_tok, m_glob, s_inv = (tokc[:, i:i + 1] for i in (0, 1, 8, 9))
    ids = lax.broadcasted_iota(jnp.int32, (1, SW), 1).astype(F32)
    for s in range(STRIPS):
        cols = slice(s * SW, (s + 1) * SW)
        scale = jnp.exp(ms_ref[:, s:s + 1] - m_glob) * s_inv
        p = e_ref[:, cols] * scale
        p = jnp.where(ids == tgt - float(s * SW), p - 1.0, p)
        q = (w_tok * p).astype(BF)
        q_s[:, cols] = q
        gw_ref[:, cols] += dot_nn(z, q)
    dz = dot_nt(q_s[...], w_ref[...])
    store_packed(dz_ref, dz, TB)
    if has_acc:
        @pl.when(pl.program_id(0) == N_DEV - 1)
        def _():
            for d in range(N_DEV):
                for c in range(VLOC // LANE):
                    pk_ref[d, c * Q:(c + 1) * Q, :] = gw_ref[Q * d:Q * d + Q, c * LANE:(c + 1) * LANE]


def head_pass2(z_all, w, tok, res, e, ms, acc):
    CHUNK_TOK = tok.shape[1]
    TB = CHUNK_TOK // N_DEV
    ZROWS = packed_rows(TB)
    in_specs = [
        lanes_spec(DIM, TB),
        whole(DIM, VLOC),
        lanes_spec(8, TB),
        lanes_spec(8, TB),
        rows_spec(TB, VLOC),
        rows_spec(TB, LANE),
    ]
    args = [z_all, w, tok, res, e, ms]
    g_shape = (DIM, VLOC) if acc is None else (N_DEV, GROWS, LANE)
    if acc is not None:
        in_specs.append(pl.BlockSpec((DIM, VLOC), lambda i: (0, 0), pipeline_mode=pl.Buffered(1)))
        args.append(acc)
    return pl.pallas_call(
        functools.partial(pass2_body, acc is not None),
        grid=(N_DEV,),
        in_specs=in_specs,
        out_specs=[
            rows_spec(1, ZROWS, LANE),
            pl.BlockSpec(g_shape, lambda i: tuple(0 * d for d in g_shape), pipeline_mode=pl.Buffered(1)),
        ],
        out_shape=[
            jax.ShapeDtypeStruct((N_DEV, ZROWS, LANE), F32),
            jax.ShapeDtypeStruct(g_shape, F32),
        ],
        scratch_shapes=[pltpu.VMEM((TB, VLOC), BF)] + ([] if acc is None else [pltpu.VMEM((DIM, VLOC), F32)]),
        compiler_params=pltpu.CompilerParams(vmem_limit_bytes=VMEM_LIMIT),
        cost_estimate=pl.CostEstimate(flops=4 * CHUNK_TOK * DIM * VLOC, bytes_accessed=4 * CHUNK_TOK * VLOC, transcendentals=0),
        name='head_pass2',
    )(*args)


def bwd_body(top, off, masks, n_in, *refs):
    h_ref, p_ref = refs[:2]
    if top:
        t_ref, d0_ref, d1_ref = refs[2:5]
    else:
        g_ref = refs[2]
    go_ref, buf_ref = refs[n_in:n_in + 2]
    scratch = refs[n_in + 2:]
    moves = []
    if masks:
        me = lax.axis_index(AXIS)
        pos = [me // w % 2 for w in (1, 2, 4, 8)]
        gp_ref = refs[n_in - 1 if top else n_in - 2]
        ga_ref, *scratch = scratch
        *scratch, send, recv, local = scratch
        barrier = pltpu.get_barrier_semaphore()
        mates = [me + sum(2**b * (1 - 2 * pos[b]) for b in range(4) if m >> b & 1) for m in masks]
        for j in mates:
            pl.semaphore_signal(barrier, inc=1, device_id=(j,), device_id_type=MESH)
        pl.semaphore_wait(barrier, len(masks))
        for i, j in enumerate(mates):
            moves.append(pltpu.make_async_remote_copy(
                src_ref=gp_ref.at[j], dst_ref=ga_ref.at[me], send_sem=send.at[i], recv_sem=recv.at[i],
                device_id=(j,), device_id_type=MESH))
        if top:
            moves.append(pltpu.make_async_copy(gp_ref.at[me], ga_ref.at[me], local))
        for move in moves:
            move.start()
    wg_ref, wu_ref, wd_ref, n_s, k_s, a_s, du_s, dv_s, pk_s, sem = scratch
    unpack_weights(p_ref, 0, wg_ref, wu_ref, wd_ref)

    for i, (lo, tb) in enumerate(SPLITS):
        rows = slice(lo, lo + tb)
        h = h_ref[rows, :].astype(F32)
        r = inv_rms_of(h)
        n = (h * r).astype(BF)
        if top:
            g = norm_grad(t_ref[rows, :].astype(F32), unpack_rows((d0_ref, d1_ref)[i], tb))
        else:
            g = g_ref[rows, :]
        k = g.astype(BF)
        u = dot_nn(n, wg_ref[...])
        v = dot_nn(n, wu_ref[...])
        e = dot_nt(k, wd_ref[...])
        sg = jax.nn.sigmoid(u)
        us = u * sg
        a_s[rows, :] = (us * v).astype(BF)
        du = (e * v * sg * (1.0 + u * (1.0 - sg))).astype(BF)
        dv = (e * us).astype(BF)
        n_s[rows, :] = n
        k_s[rows, :] = k
        du_s[rows, :] = du
        dv_s[rows, :] = dv
        dn = dot_nt(du, wg_ref[...]) + dot_nt(dv, wu_ref[...])
        go_ref[rows, :] = (g + r * dn - h * (r * r * r) * jnp.mean(h * dn, axis=-1, keepdims=True)).astype(go_ref.dtype)

    n = n_s[...]
    k = k_s[...]
    for c in range(6):
        gg = dot_tn(n, du_s[:, c * 256:(c + 1) * 256])
        gu = dot_tn(n, dv_s[:, c * 256:(c + 1) * 256])
        for j in range(2):
            base = (2 * c + j) * Q2
            for d in range(N_DEV):
                pk_s[d, base:base + Q, :] = gg[Q * d:Q * d + Q, j * LANE:(j + 1) * LANE]
                pk_s[d, base + Q:base + Q2, :] = gu[Q * d:Q * d + Q, j * LANE:(j + 1) * LANE]
    copy_a = pltpu.make_async_copy(pk_s.at[:, pl.ds(0, A0), :], buf_ref.at[:, pl.ds(off, A0), :], sem.at[0])
    copy_a.start()
    for c in range(4):
        gd = dot_tn(a_s[:, c * 384:(c + 1) * 384], k)
        for j in range(4):
            d = c * 4 + j
            x = gd[PD * j:PD * j + PD, :]
            for b in range(4):
                pk_s[d, A0 + PD * b:A0 + PD * b + PD, :] = x[:, LANE * b:LANE * b + LANE]
            pk_s[d, TL0:1296, :] = jnp.concatenate([x[:PH, D4:], x[PH:, D4:]], axis=1)
    copy_b = pltpu.make_async_copy(pk_s.at[:, pl.ds(A0, 432), :], buf_ref.at[:, pl.ds(off + A0, 432), :], sem.at[1])
    copy_b.start()
    copy_a.wait()
    copy_b.wait()
    for move in moves:
        move.wait()


def block_backward(h, packs, wslot, g_args, buf, slot, slots, out_dtype, masks=(), moved=(), cid=None):
    top = len(g_args) == 3
    args = [h, packs, *g_args]
    in_specs = [whole(TOK, DIM), pl.BlockSpec((N_DEV, 1, PROWS, LANE), lambda i: (0, wslot, 0, 0))]
    in_specs += [whole(*x.shape) for x in g_args]
    out_specs = [whole(TOK, DIM), HB]
    out_shape = [jax.ShapeDtypeStruct((TOK, DIM), out_dtype), jax.ShapeDtypeStruct((N_DEV, slots * PROWS, LANE), F32)]
    scratch = W_SCRATCH + [
        pltpu.VMEM((TOK, DIM), BF), pltpu.VMEM((TOK, DIM), BF), pltpu.VMEM((TOK, FFN), BF),
        pltpu.VMEM((TOK, FFN), BF), pltpu.VMEM((TOK, FFN), BF), pltpu.VMEM((N_DEV, PROWS, LANE), F32),
        pltpu.SemaphoreType.DMA((2,)),
    ]
    aliases = {}
    if buf is not None:
        aliases[len(args)] = 1
        args.append(buf)
        in_specs.append(HB)
    if masks:
        sems = pltpu.SemaphoreType.DMA((len(masks),))
        scratch += [sems, sems, pltpu.SemaphoreType.DMA]
        if len(moved) == 2:
            aliases[len(args) + 1] = 2
        args += moved
        in_specs += [HB] * len(moved)
        out_specs.append(HB)
        out_shape.append(jax.ShapeDtypeStruct(moved[0].shape, F32))
    return pl.pallas_call(
        functools.partial(bwd_body, top, slot * PROWS, masks, len(args)),
        grid=(1,),
        in_specs=in_specs,
        out_specs=out_specs,
        out_shape=out_shape,
        scratch_shapes=scratch,
        input_output_aliases=aliases,
        compiler_params=pltpu.CompilerParams(vmem_limit_bytes=VMEM_LIMIT, collective_id=cid, has_side_effects=bool(masks)),
        cost_estimate=pl.CostEstimate(flops=16 * TOK * DIM * FFN, bytes_accessed=24 * 2**20, transcendentals=TOK * FFN),
        name='block_backward',
    )(*args)


def head_unpack_body(p_ref, o_ref):
    for c in range(VLOC // LANE):
        o_ref[:, c * LANE:(c + 1) * LANE] = p_ref[0, c * Q:(c + 1) * Q, :]


def unpack_head(p):
    return pl.pallas_call(
        head_unpack_body,
        grid=(N_DEV,),
        in_specs=[rows_spec(1, GROWS, LANE)],
        out_specs=lanes_spec(Q, VLOC),
        out_shape=jax.ShapeDtypeStruct((Q, VOCAB), F32),
        name='unpack_head',
    )(p)


def cube_body(pieces, x_ref, o_ref, own, r0, r1, r2, r3, send, recv, local):
    me = lax.axis_index(AXIS)
    pos = [me // 8, me // 4 % 2, me // 2 % 2, me % 2]
    weight = (8, 4, 2, 1)
    mate = [me + w * (1 - 2 * p) for w, p in zip(weight, pos)]
    sem = pltpu.get_barrier_semaphore()
    for j in mate:
        pl.semaphore_signal(sem, inc=1, device_id=(j,), device_id_type=MESH)
    pl.semaphore_wait(sem, 4)
    core = pos[3]
    size = o_ref.shape[0] // (3 * pieces)
    units = [(k, (k + 3 * p) * size) for p in range(pieces) for k in range(3)]

    def pick(ref, k, stage, rows, flip):
        index = [slice(None)] * 3
        for j in range(stage):
            d = (k + j) % 3
            index[d] = pos[d]
        d = (k + stage) % 3
        index[d] = 1 - pos[d] if flip else pos[d]
        return ref.at[(*index, rows)]

    def landing(k, stage, rows):
        return (r1.at[:, :, rows], r2.at[:, rows], r3.at[rows])[stage]

    def first(u):
        k, base = units[u]
        rows = pl.ds(base, size)
        out = pltpu.make_async_remote_copy(
            src_ref=x_ref.at[:, :, :, 1 - core, rows], dst_ref=r0.at[:, :, :, rows], send_sem=send.at[0, u],
            recv_sem=recv.at[0, u], device_id=(mate[3],), device_id_type=MESH)
        return out, pltpu.make_async_copy(x_ref.at[:, :, :, core, rows], own.at[:, :, :, rows], local.at[u])

    def later(u, stage):
        k, base = units[u]
        rows = pl.ds(base, size)
        return pltpu.make_async_remote_copy(
            src_ref=pick(own, k, stage, rows, True), dst_ref=landing(k, stage, rows), send_sem=send.at[stage + 1, u],
            recv_sem=recv.at[stage + 1, u], device_id=(mate[(k + stage) % 3],), device_id_type=MESH)

    def add(dst, src):
        step = PH

        def body(i, carry):
            rows = pl.ds(pl.multiple_of(i * step, step), step)
            lead = (slice(None),) * (len(dst.shape) - 2)
            dst[(*lead, rows)] += src[(*lead, rows)]
            return carry

        lax.fori_loop(0, size // step, body, 0)

    many = range(len(units))
    for u in many:
        for copy in first(u):
            copy.start()
    for stage in range(4):
        for u in many:
            k, base = units[u]
            rows = pl.ds(base, size)
            if stage == 0:
                out, loc = first(u)
                loc.wait()
                out.wait_recv()
                add(own.at[:, :, :, rows], r0.at[:, :, :, rows])
            else:
                later(u, stage - 1).wait_recv()
                add(pick(own, k, stage - 1, rows, False), landing(k, stage - 1, rows))
            if stage < 3:
                if u > 0:
                    later(u - 1, stage).start()
                if u == many[-1]:
                    later(u, stage).start()
            else:
                o_ref[rows, :] = own[(*pos[:3], rows)]
    for u in many:
        first(u)[0].wait_send()
        for stage in range(3):
            later(u, stage).wait_send()


def cube_reduce_scatter(x, pieces, cid):
    rows = x.shape[1]
    units = 3 * pieces
    return pl.pallas_call(
        functools.partial(cube_body, pieces),
        in_specs=[HB],
        out_specs=VM,
        out_shape=jax.ShapeDtypeStruct((rows, LANE), F32),
        scratch_shapes=[
            pltpu.VMEM((2, 2, 2, rows, LANE), F32), pltpu.VMEM((2, 2, 2, rows, LANE), F32), pltpu.VMEM((2, 2, rows, LANE), F32),
            pltpu.VMEM((2, rows, LANE), F32), pltpu.VMEM((rows, LANE), F32),
            pltpu.SemaphoreType.DMA((4, units)), pltpu.SemaphoreType.DMA((4, units)), pltpu.SemaphoreType.DMA((units,)),
        ],
        compiler_params=pltpu.CompilerParams(collective_id=cid, has_side_effects=True, vmem_limit_bytes=VMEM_LIMIT),
        cost_estimate=pl.CostEstimate(flops=50 * 10**9, bytes_accessed=2**20, transcendentals=0),
        name='cube_reduce_scatter',
    )(x.reshape(2, 2, 2, 2, rows, LANE))


def unpack_body(has_prev, p_ref, *refs):
    gg_ref, gu_ref, gd_ref = refs[3:] if has_prev else refs
    for c in range(12):
        gg_ref[0, :, c * LANE:(c + 1) * LANE] = p_ref[c * Q2:c * Q2 + Q, :]
        gu_ref[0, :, c * LANE:(c + 1) * LANE] = p_ref[c * Q2 + Q:c * Q2 + Q2, :]
    for b in range(4):
        gd_ref[0, :, b * LANE:(b + 1) * LANE] = p_ref[A0 + PD * b:A0 + PD * b + PD, :]
    tail = p_ref[TL0:1296, :]
    gd_ref[0, 0:PH, D4:DIM] = tail[:, :HL]
    gd_ref[0, PH:PD, D4:DIM] = tail[:, HL:]


def unpack_grads(packed, group, prev):
    prev = list(prev or ())
    back = lambda i: (group[0] - i, 0, 0)
    return pl.pallas_call(
        functools.partial(unpack_body, bool(prev)),
        grid=(len(group),),
        in_specs=[rows_spec(PROWS, LANE)] + [HB] * len(prev),
        out_specs=[
            pl.BlockSpec((1, Q, FFN), back),
            pl.BlockSpec((1, Q, FFN), back),
            pl.BlockSpec((1, PD, DIM), back),
        ],
        out_shape=[
            jax.ShapeDtypeStruct((LAYERS, Q, FFN), F32),
            jax.ShapeDtypeStruct((LAYERS, Q, FFN), F32),
            jax.ShapeDtypeStruct((LAYERS, PD, DIM), F32),
        ],
        input_output_aliases={1 + i: i for i in range(len(prev))},
        name='unpack_grads',
    )(packed, *prev)


def pack_body(wg_ref, wu_ref, wd_ref, p_ref):
    for c in range(12):
        p_ref[0, c * Q2:c * Q2 + Q, :] = wg_ref[0, :, c * LANE:(c + 1) * LANE]
        p_ref[0, c * Q2 + Q:c * Q2 + Q2, :] = wu_ref[0, :, c * LANE:(c + 1) * LANE]
    for b in range(4):
        p_ref[0, A0 + PD * b:A0 + PD * b + PD, :] = wd_ref[0, :, b * LANE:(b + 1) * LANE]
    p_ref[0, TL0:1296, :] = jnp.concatenate([wd_ref[0, 0:PH, D4:DIM], wd_ref[0, PH:PD, D4:DIM]], axis=1)


def pack_weights(wg, wu, wd):
    return pl.pallas_call(
        pack_body,
        grid=(LAYERS,),
        in_specs=[
            rows_spec(1, Q, FFN),
            rows_spec(1, Q, FFN),
            rows_spec(1, PD, DIM),
        ],
        out_specs=rows_spec(1, PROWS, LANE),
        out_shape=jax.ShapeDtypeStruct((LAYERS, PROWS, LANE), BF),
        name='pack_weights',
    )(wg, wu, wd)


def unpack_weights(p_ref, slot, wg_s, wu_s, wd_s):
    for d in range(N_DEV):
        for c in range(12):
            cols = slice(c * LANE, (c + 1) * LANE)
            wg_s[Q * d:Q * d + Q, cols] = p_ref[d, slot, c * Q2:c * Q2 + Q, :]
            wu_s[Q * d:Q * d + Q, cols] = p_ref[d, slot, c * Q2 + Q:c * Q2 + Q2, :]
        for b in range(4):
            wd_s[PD * d:PD * d + PD, LANE * b:LANE * b + LANE] = p_ref[d, slot, A0 + PD * b:A0 + PD * b + PD, :]
        tail = p_ref[d, slot, TL0:1296, :]
        wd_s[PD * d:PD * d + PH, D4:DIM] = tail[:, :HL]
        wd_s[PD * d + PH:PD * d + PD, D4:DIM] = tail[:, HL:]


PEERS = ((1, 15), (3, 5, 9), (2, 4, 8, 14), (7, 11, 13), (6, 10, 12))
GROUPS = ((4, 3), (2, 1, 0))


def solution(mesh):
    def device_step(hidden, w_gate, w_up, w_down, w_out, targets, loss_mask):
        me = lax.axis_index(AXIS)
        gather = functools.partial(lax.all_gather, axis_name=AXIS)
        barrier = lax.optimization_barrier
        lab = jnp.concatenate([targets.astype(F32)[None], loss_mask.astype(F32)[None], jnp.zeros((6, TOK), F32)], axis=0)
        packs = pack_weights(w_gate, w_up, w_down)
        packs, lab = barrier((packs, lab))
        pack_top = gather(packs[4:])
        lab, w_vocab = start_exchange(lab, w_out)
        pack_top, w_vocab, lab = barrier((pack_top, w_vocab, lab))
        w_vocab = w_vocab.reshape(DIM, VLOC)
        t, *z_packed = top_forward(hidden[4], pack_top)

        mask = lab[:, 1, :]
        w_tok = mask / jnp.sum(mask)
        tgt = lab[:, 0, :] - (me * VLOC).astype(F32)
        w_own = lax.dynamic_slice(w_tok, (me, 0), (1, TOK))

        z_all = [lax.all_gather(z, AXIS, tiled=True) for z in z_packed]
        rest = gather(packs[:4])
        hs = [hidden[l] for l in range(LAYERS)]
        acc, loss, dz_own = None, jnp.zeros((), F32), []
        for c, (lo, tb) in enumerate(SPLITS):
            sl = slice(lo, lo + tb)
            CHUNK_TOK = tb * N_DEV
            zero = jnp.zeros((6, CHUNK_TOK), F32)
            tok = jnp.concatenate([tgt[:, sl].reshape(1, CHUNK_TOK), w_tok[:, sl].reshape(1, CHUNK_TOK), zero], axis=0)
            if c == 0:
                tok, *hs = barrier((tok, *hs))
            if c == 1:
                tok, acc, rest = barrier((tok, acc, rest))
            e, ms, st, z_t = head_pass1(z_all[c], w_vocab, tok)
            res = exchange_stats(st, w_own[:, sl], 2 + c)
            loss = loss + jnp.sum(res[2])
            dz, acc = head_pass2(z_t, w_vocab, tok, res, e, ms, acc)
            if c == 1:
                dz, dz_own[0] = barrier((dz, dz_own[0]))
                dz_own.append(cube_reduce_scatter(dz, 2, 4))
            else:
                dz_own.append(lax.psum_scatter(dz, AXIS, scatter_dimension=0, tiled=False))
        g_args = [t, *dz_own]
        bufs, moved = [], [acc]
        for group in GROUPS:
            buf = None
            for i, l in enumerate(group):
                pk, ws = (pack_top, 0) if l == 4 else (rest, l)
                args = (hs[l], pk, ws, g_args, buf, i, len(group), BF if l == 0 else F32)
                g, buf, got = block_backward(*args, PEERS[l], moved, l + 6)
                moved = [acc, got]
                g_args = [g]
            bufs.append(buf)
        grad_out = unpack_head(moved[1])
        red = lax.psum_scatter(bufs[0], AXIS, scatter_dimension=0, tiled=False)
        bufs[1], grad_out = barrier((bufs[1], grad_out))
        red_low = cube_reduce_scatter(bufs[1], 3, 5)
        red, red_low = barrier((red, red_low))
        outs = unpack_grads(red, GROUPS[0], None)
        grad_gate, grad_up, grad_down = unpack_grads(red_low, GROUPS[1], outs)
        return grad_gate, grad_up, grad_down, grad_out, g, loss

    stacked = P(None, AXIS, None)
    row = P(AXIS, None)
    return jax.shard_map(device_step, mesh=mesh, in_specs=(stacked, stacked, stacked, stacked, row, P(AXIS), P(AXIS)), out_specs=(stacked, stacked, stacked, row, row, P()), check_vma=False)
```
